16 devices in a mesh: dp: 4 (over y, z, core), tp: 4 (over x).
Axes of the slice: x: 4, y: 2, z: 1, core: 2. Of those that a mesh axis runs over, the one named last changes fastest.
The devices are a block of a 4x4x8 slice.
Arguments:
- x: bfloat16 [8192, 2048], P(('dp', 'tp')), parts along dimension 0
- gain_a: bfloat16 [2048], replicated
- wq: bfloat16 [2048, 2048], P(None, 'tp')
- wk: bfloat16 [2048, 2048], P(None, 'tp')
- wv: bfloat16 [2048, 2048], P(None, 'tp')
- wo: bfloat16 [2048, 2048], P('tp')
- gain_m: bfloat16 [2048], replicated
- w_gate: bfloat16 [2048, 8192], P(None, 'tp')
- w_up: bfloat16 [2048, 8192], P(None, 'tp')
- w_down: bfloat16 [8192, 2048], P('tp')
Outputs:
- output: bfloat16 [8192, 2048], P(('dp', 'tp')), parts along dimension 0
There are 4 independent parts. The reference program is written for one: setup_inputs(seed, part) draws one part's arguments, and reference() takes and returns one part's arrays. A program takes and returns all parts, laid end to end along the dimension named above; an argument that names none is the same for every part.
All inputs are finite; a program needn't handle non-finite values.
Results may differ from the reference program's by a relative error of at most 0.017.
Values are sent between devices in bfloat16 or wider.
A program may use at most 768 MiB of HBM per device.

```python
import jax
import jax.numpy as jnp
from jax import lax

ROWS = 2048
D = 2048
HEADS = 16
KV_HEADS = 16
HEAD = 128
FF = 8192
THETA = 10000


def setup_inputs(seed: int = 0, part: int = 0) -> dict:
    kx, kn, kq, kk, kv, ko, km, kg, ku, kd = jax.random.split(jax.random.key(seed), 10)

    def weights(key, rows, columns):
        return jax.random.normal(key, (rows, columns), jnp.float32) * rows**-0.5

    drawn = {
        "x": jax.random.normal(jax.random.fold_in(kx, part), (ROWS, D), jnp.float32),
        "gain_a": 1 + 0.1 * jax.random.normal(kn, (D,), jnp.float32),
        "wq": 2 * weights(kq, D, HEADS * HEAD),
        "wk": 2 * weights(kk, D, KV_HEADS * HEAD),
        "wv": 4 * weights(kv, D, KV_HEADS * HEAD),
        "wo": weights(ko, HEADS * HEAD, D),
        "gain_m": 1 + 0.1 * jax.random.normal(km, (D,), jnp.float32),
        "w_gate": weights(kg, D, FF),
        "w_up": weights(ku, D, FF),
        "w_down": 2 * weights(kd, FF, D),
    }
    return {k: v.astype(jnp.bfloat16) for k, v in drawn.items()}


def normed(x, gain):
    wide = x.astype(jnp.float32)
    scale = lax.rsqrt(jnp.mean(wide * wide, -1, keepdims=True) + 1e-6)
    return (wide * scale * gain.astype(jnp.float32)).astype(jnp.bfloat16)


def turned(t, place, theta):
    half = t.shape[-1] // 2
    angle = place.astype(jnp.float32)[:, None] * theta ** (-jnp.arange(half, dtype=jnp.float32) / half)
    cos, sin = jnp.cos(angle)[:, None], jnp.sin(angle)[:, None]
    a, b = t[..., :half].astype(jnp.float32), t[..., half:].astype(jnp.float32)
    return jnp.concatenate([a * cos - b * sin, b * cos + a * sin], -1).astype(jnp.bfloat16)


def matmul(a, w):
    return jnp.dot(a, w, preferred_element_type=jnp.float32).astype(jnp.bfloat16)


def einsum(form, a, b):
    return jnp.einsum(form, a.astype(jnp.float32), b.astype(jnp.float32))


def attention(q, k, v):
    scores = einsum("tgsd,ugd->gstu", q, k) * q.shape[-1] ** -0.5
    token = jnp.arange(q.shape[0])
    scores = jnp.where(token[:, None] >= token, scores, -jnp.inf)
    weights = jax.nn.softmax(scores, -1).astype(jnp.bfloat16)
    return einsum("gstu,ugd->tgsd", weights, v).astype(jnp.bfloat16)


def reference(x, gain_a, wq, wk, wv, wo, gain_m, w_gate, w_up, w_down):
    a, place = normed(x, gain_a), jnp.arange(ROWS)
    q = turned(matmul(a, wq).reshape(ROWS, HEADS, HEAD), place, THETA).reshape(ROWS, KV_HEADS, -1, HEAD)
    k = turned(matmul(a, wk).reshape(ROWS, KV_HEADS, HEAD), place, THETA)
    v = matmul(a, wv).reshape(ROWS, KV_HEADS, HEAD)
    seen = attention(q, k, v).reshape(ROWS, HEADS * HEAD)
    h = (x.astype(jnp.float32) + jnp.dot(seen, wo, preferred_element_type=jnp.float32)).astype(jnp.bfloat16)
    b = normed(h, gain_m)
    gate = jnp.dot(b, w_gate, preferred_element_type=jnp.float32)
    up = jnp.dot(b, w_up, preferred_element_type=jnp.float32)
    hidden = (jax.nn.silu(gate) * up).astype(jnp.bfloat16)
    return (h.astype(jnp.float32) + jnp.dot(hidden, w_down, preferred_element_type=jnp.float32)).astype(jnp.bfloat16)
```

```python
import functools

import jax
import jax.numpy as jnp
import numpy as np
from jax import lax
from jax.experimental import pallas as pl
from jax.experimental.pallas import tpu as pltpu
from jax.sharding import PartitionSpec as P

HEAD = 128
THETA = 10000
NEG = -1e30
HIDDEN = 2 * NEG
LOG2E = 1.4426950408889634
VMEM = 67043328
TILE = 512
F32, BF16 = jnp.float32, jnp.bfloat16
OWN, LEFT, RIGHT, OPP = 0, 1, 2, 3


def _dot(a, b, ca=1, cb=0):
    return lax.dot_general(a, b, (((ca,), (cb,)), ((), ())), preferred_element_type=F32)


def _ring():
    n = lax.axis_size("tp")
    me = lax.axis_index("tp")
    return me, lax.rem(me + n - 1, n), lax.rem(me + 1, n), lax.rem(me + 2, n)


def _greet(peers):
    barrier = pltpu.get_barrier_semaphore()
    for peer in peers:
        pl.semaphore_signal(barrier, inc=1, device_id=peer, device_id_type=pl.DeviceIdType.MESH)
    pl.semaphore_wait(barrier, len(peers))


def _norm(src, gain_ref, dst, at, rows, step=32):
    gain = gain_ref[...].astype(F32)

    @pl.loop(0, rows // step)
    def _(i):
        here = pl.ds(pl.multiple_of(at + i * step, step), step)
        wide = src[here, :].astype(F32)
        scale = lax.rsqrt(jnp.mean(wide * wide, -1, keepdims=True) + 1e-6)
        dst[here, :] = (wide * scale * gain).astype(BF16)


class _Copies:
    def __init__(self, send, recv):
        self.send, self.recv, self.n, self.all = send, recv, 0, []

    def __call__(self, src, dst, peer):
        copy = pltpu.make_async_remote_copy(src_ref=src, dst_ref=dst, send_sem=self.send.at[self.n], recv_sem=self.recv.at[self.n],
                                            device_id=peer, device_id_type=pl.DeviceIdType.MESH)
        self.n += 1
        self.all.append(copy)
        return copy


def _gather(copies, tok, half, right, left):
    h = [pl.ds(0, half), pl.ds(half, half)]
    own_r = [copies(tok.at[OWN, h[i]], tok.at[LEFT, h[i]], right) for i in (0, 1)]
    own_l = [copies(tok.at[OWN, h[i]], tok.at[RIGHT, h[i]], left) for i in (0, 1)]
    fwd_r = copies(tok.at[LEFT, h[0]], tok.at[OPP, h[0]], right)
    fwd_l = copies(tok.at[RIGHT, h[1]], tok.at[OPP, h[1]], left)
    return own_r, own_l, fwd_r, fwd_l


MLP_PARTS = 4


def _mlp(h_ref, gain_ref, wg_hbm, wu_hbm, wd_hbm, y_ref, tok, wg, wu, wd, hid, own, mid, dsend, osend, ssend, drecv, orecv, srecv,
         wsem, ssem, rsem):
    me, to_left, to_right, _ = _ring()
    right, left = {"tp": to_right}, {"tp": to_left}
    rows, width = h_ref.shape
    half = rows // 2
    part = half // MLP_PARTS
    ff = wg.shape[1]

    def load(i, j):
        hbm, ref = ((wg_hbm, wg), (wu_hbm, wu), (wd_hbm, wd))[i]
        cols = pl.ds(pl.multiple_of(j * TILE, TILE), TILE)
        return pltpu.make_async_copy(hbm.at[:, cols], ref.at[:, cols], wsem.at[i, j])

    for j in range(ff // TILE):
        load(0, j).start()
        load(1, j).start()
    for j in range(width // TILE):
        load(2, j).start()
    _greet((right, left))

    copies = _Copies(ssem, rsem)
    own_r, own_l, fwd_r, fwd_l = _gather(copies, tok, half, right, left)
    _norm(h_ref, gain_ref, tok.at[OWN], 0, half)
    own_r[0].start()
    _norm(h_ref, gain_ref, tok.at[OWN], half, half)
    own_l[1].start()
    own_r[1].start()
    own_l[0].start()

    def term(slot, i, store, first=False):
        here = pl.ds(i * half, half)

        @pl.loop(0, ff // TILE)
        def _(j):
            cols = pl.ds(pl.multiple_of(j * TILE, TILE), TILE)
            if first:
                load(0, j).wait()
                load(1, j).wait()
            gate = _dot(tok[slot, here, :], wg[:, cols])
            up = _dot(tok[slot, here, :], wu[:, cols])
            hid[:, cols] = (jax.nn.silu(gate) * up).astype(BF16)

        @pl.loop(0, width // TILE)
        def _(j):
            cols = pl.ds(pl.multiple_of(j * TILE, TILE), TILE)
            if first:
                load(2, j).wait()
            store(cols, _dot(hid[...], wd[:, cols]))

    def keep(i):
        here = pl.ds(i * half, half)

        def store(cols, t):
            own[here, cols] = h_ref[here, cols].astype(F32) + t

        return store

    def put(ref, side):
        def store(cols, t):
            ref[side, :, cols] = t.astype(ref.dtype)

        return store

    term(OWN, 0, keep(0), first=True)
    term(OWN, 1, keep(1))

    peer = (right, left)
    direct = [copies(dsend.at[s], drecv.at[s], peer[s]) for s in (0, 1)]
    piece = [pl.ds(p * part, part) for p in range(MLP_PARTS)]
    opp = [[copies(osend.at[s, at], orecv.at[s, at], peer[s]) for at in piece] for s in (0, 1)]
    total = [[copies(ssend.at[s, at], srecv.at[s, at], peer[s]) for at in piece] for s in (0, 1)]

    own_r[0].wait_recv()
    fwd_r.start()
    own_l[1].wait_recv()
    fwd_l.start()
    term(LEFT, 0, put(dsend, 1))
    direct[1].start()
    term(RIGHT, 1, put(dsend, 0))
    direct[0].start()
    own_r[1].wait_recv()
    term(LEFT, 1, put(mid, 1))
    own_l[0].wait_recv()
    term(RIGHT, 0, put(mid, 0))
    fwd_r.wait_recv()
    term(OPP, 0, put(osend, 0))
    for c in opp[0]:
        c.start()
    fwd_l.wait_recv()
    term(OPP, 1, put(osend, 1))
    for c in opp[1]:
        c.start()
    for p in range(MLP_PARTS):
        for s in (0, 1):
            opp[s][p].wait_recv()
            ssend[s, piece[p]] = (mid[s, piece[p]] + orecv[s, piece[p]].astype(F32)).astype(BF16)
            total[s][p].start()
    for s in (0, 1):
        direct[s].wait_recv()
    for p in range(MLP_PARTS):
        for s in (0, 1):
            total[s][p].wait_recv()
            here = pl.ds(s * half + p * part, part)
            y_ref[here, :] = (own[here, :] + srecv[s, piece[p]].astype(F32) + drecv[1 - s, piece[p]].astype(F32)).astype(BF16)
    for c in copies.all:
        c.wait_send()


def mlp_half(h, gain, w_gate, w_up, w_down):
    rows, width = h.shape
    ff = w_gate.shape[1]
    half = rows // 2
    n = 8 + 4 * MLP_PARTS
    anywhere, here = pl.BlockSpec(memory_space=pl.ANY), pl.BlockSpec(memory_space=pltpu.VMEM)
    halves = lambda kind: pltpu.VMEM((2, half, width), kind)
    return pl.pallas_call(
        _mlp,
        out_shape=jax.ShapeDtypeStruct((rows, width), BF16),
        in_specs=[here, here, anywhere, anywhere, anywhere],
        out_specs=here,
        scratch_shapes=[pltpu.VMEM((4, rows, width), BF16), pltpu.VMEM((width, ff), BF16), pltpu.VMEM((width, ff), BF16),
                        pltpu.VMEM((ff, width), BF16), pltpu.VMEM((half, ff), BF16), pltpu.VMEM((rows, width), F32), halves(F32),
                        halves(BF16), halves(BF16), halves(BF16), halves(BF16), halves(BF16), halves(BF16),
                        pltpu.SemaphoreType.DMA((3, max(ff, width) // TILE)), pltpu.SemaphoreType.DMA((n,)), pltpu.SemaphoreType.DMA((n,))],
        compiler_params=pltpu.CompilerParams(collective_id=1, has_side_effects=True, vmem_limit_bytes=VMEM),
        cost_estimate=pl.CostEstimate(flops=24 * rows * width * ff, transcendentals=4 * rows * ff, bytes_accessed=6 * width * ff),
        name="mlp_half",
    )(h, gain.reshape(1, -1), w_gate, w_up, w_down)


def _attention(x_ref, gain_ref, turn_ref, wq_hbm, wk_hbm, wv_hbm, wo_hbm, h_ref, tok, w, wo, table, q, k, v, top_s, mix_s, out, got, relay, acc,
               wsem, ssem, rsem):
    me, to_left, to_right, to_opp = _ring()
    dp = lax.axis_index("dp")
    core = lax.rem(dp, 2)
    right, left, other = {"tp": to_right}, {"tp": to_left}, {"dp": dp + 1 - 2 * core}
    rows, width = x_ref.shape
    half = rows // 2
    heads = q.shape[0]
    block_of = (me, to_left, to_right, to_opp)

    loads = [pltpu.make_async_copy(hbm, w.at[i], wsem.at[i]) for i, hbm in enumerate((wq_hbm, wk_hbm, wv_hbm))]
    loads.append(pltpu.make_async_copy(wo_hbm, wo.at[OWN], wsem.at[3]))
    for c in loads:
        c.start()
    _greet((right, left, other))

    copies = _Copies(ssem, rsem)
    own_r, own_l, fwd_r, fwd_l = _gather(copies, tok, half, right, left)
    _norm(x_ref, gain_ref, tok.at[OWN], 0, half)
    own_r[0].start()
    _norm(x_ref, gain_ref, tok.at[OWN], half, half)
    own_l[1].start()
    own_r[1].start()
    own_l[0].start()

    def angles(slot, i, t):
        place = lax.broadcasted_iota(jnp.int32, (half, HEAD), 0) + (block_of[slot] * rows + i * half)
        angle = place.astype(F32) * turn_ref[...]
        sign = jnp.where(lax.broadcasted_iota(jnp.int32, (half, HEAD), 1) < HEAD // 2, -1.0, 1.0)
        table[t, 0] = jnp.cos(angle)
        table[t, 1] = jnp.sin(angle) * sign

    def project(slot, i, t, first=False):
        here = pl.ds(i * half, half)
        there = pl.ds(pl.multiple_of(block_of[slot] * rows + i * half, half), half)
        for n, ref in enumerate((q, k, v)):
            if first:
                loads[n].wait()
            full = _dot(tok[slot, here, :], w[n]).astype(BF16)
            for a in range(heads):
                one = full[:, a * HEAD : (a + 1) * HEAD]
                if n < 2:
                    wide = one.astype(F32)
                    one = (wide * table[t, 0] + pltpu.roll(wide, HEAD // 2, 1) * table[t, 1]).astype(BF16)
                ref[a, there, :] = one

    angles(OWN, 0, 0)
    angles(OWN, 1, 1)
    project(OWN, 0, 0, first=True)
    project(OWN, 1, 1)
    angles(LEFT, 0, 0)
    angles(RIGHT, 1, 1)
    own_r[0].wait_recv()
    fwd_r.start()
    own_l[1].wait_recv()
    fwd_l.start()
    project(LEFT, 0, 0)
    project(RIGHT, 1, 1)
    angles(LEFT, 1, 0)
    angles(RIGHT, 0, 1)
    own_r[1].wait_recv()
    project(LEFT, 1, 0)
    own_l[0].wait_recv()
    project(RIGHT, 0, 1)
    angles(OPP, 0, 0)
    angles(OPP, 1, 1)

    mine = pl.multiple_of(core * half, half)
    quarter = half // 2
    first_q, second_q = pl.ds(mine, quarter), pl.ds(pl.multiple_of(mine + quarter, quarter), quarter)
    mine = pl.ds(mine, half)
    wo_r = copies(wo.at[OWN, mine], wo.at[LEFT, mine], right)
    wo_l = copies(wo.at[OWN, mine], wo.at[RIGHT, mine], left)
    wo_fr = copies(wo.at[LEFT, first_q], wo.at[OPP, first_q], right)
    wo_fl = copies(wo.at[RIGHT, second_q], wo.at[OPP, second_q], left)
    wo_x = [copies(wo.at[s, at], wo.at[s, at], other) for s, at in ((LEFT, mine), (RIGHT, mine), (OPP, first_q), (OPP, second_q))]

    fwd_r.wait_recv()
    fwd_l.wait_recv()
    loads[3].wait()
    wo_r.start()
    wo_l.start()
    project(OPP, 0, 0)
    project(OPP, 1, 1)

    e = HEAD**-0.5 * LOG2E
    ones = jnp.ones((8, rows), BF16)

    def attend(slot):
        block = block_of[slot]
        mine = pl.ds(pl.multiple_of(block * rows, rows), rows)
        top_s[...] = jnp.full(top_s.shape, NEG, F32)
        mix_s[...] = jnp.zeros(mix_s.shape, F32)

        def step(j, masked):
            here = pl.ds(pl.multiple_of(j * rows, rows), rows)
            scores = [_dot(k[a, here, :], q[a, mine, :], 1, 1) for a in range(heads)]
            weights, keeps = [], []
            for a, s in enumerate(scores):
                if masked:
                    s = jnp.where(lax.broadcasted_iota(jnp.int32, s.shape, 1) >= lax.broadcasted_iota(jnp.int32, s.shape, 0), s, HIDDEN)
                old = top_s[a : a + 1, :]
                top = jnp.maximum(old, s.max(axis=0, keepdims=True))
                top_s[a : a + 1, :] = top
                weights.append(jnp.exp2((s - top) * e).astype(BF16))
                keeps.append(jnp.exp2((old - top) * e))
            for a, (p, keep) in enumerate(zip(weights, keeps)):
                values = jnp.concatenate([v[a, here, :].T, ones], axis=0)
                mix_s[a] = mix_s[a] * keep + _dot(values, p)

        lax.fori_loop(0, block, lambda j, _: step(j, False), None)
        step(block, True)
        for a in range(heads):
            out[slot, :, a * HEAD : (a + 1) * HEAD] = (mix_s[a, :HEAD, :] * (1 / mix_s[a, HEAD : HEAD + 1, :])).T.astype(BF16)

    h0, h1 = pl.ds(0, half), pl.ds(half, half)
    opp_r = copies(out.at[OPP, h0], relay.at[0], right)
    opp_l = copies(out.at[OPP, h1], relay.at[1], left)
    out_l = copies(out.at[LEFT], got.at[RIGHT], left)
    out_r = copies(out.at[RIGHT], got.at[LEFT], right)
    rel_r = copies(relay.at[0], got.at[OPP, h0], right)
    rel_l = copies(relay.at[1], got.at[OPP, h1], left)

    attend(OPP)
    opp_r.start()
    opp_l.start()
    attend(LEFT)
    out_l.start()
    attend(RIGHT)
    out_r.start()
    wo_r.wait_recv()
    wo_fr.start()
    wo_l.wait_recv()
    wo_fl.start()
    wo_x[0].start()
    wo_x[1].start()
    attend(OWN)
    opp_r.wait_recv()
    rel_r.start()
    opp_l.wait_recv()
    rel_l.start()

    tiles = [pl.ds(j * TILE, TILE) for j in range(width // TILE)]
    for cols in tiles:
        acc[:, cols] = x_ref[:, cols].astype(F32) + _dot(out[OWN], wo[OWN, :, cols])
    out_l.wait_recv()
    out_r.wait_recv()
    wo_x[0].wait_recv()
    wo_x[1].wait_recv()
    for cols in tiles:
        acc[:, cols] += _dot(got[LEFT], wo[LEFT, :, cols]) + _dot(got[RIGHT], wo[RIGHT, :, cols])
    wo_fr.wait_recv()
    wo_x[2].start()
    wo_fl.wait_recv()
    wo_x[3].start()
    rel_r.wait_recv()
    rel_l.wait_recv()
    wo_x[2].wait_recv()
    wo_x[3].wait_recv()
    for cols in tiles:
        h_ref[:, cols] = (acc[:, cols] + _dot(got[OPP], wo[OPP, :, cols])).astype(BF16)
    for c in copies.all:
        c.wait_send()


def attention_half(x, gain, wq, wk, wv, wo):
    rows, width = x.shape
    columns = wq.shape[1]
    heads, half = columns // HEAD, rows // 2
    n = 20
    anywhere, here = pl.BlockSpec(memory_space=pl.ANY), pl.BlockSpec(memory_space=pltpu.VMEM)
    low = HEAD // 2
    turn = np.float32(THETA) ** (-np.arange(low, dtype=np.float32) / np.float32(low))
    turn = jnp.asarray(np.tile(turn, 2)[None])
    tokens = 4 * rows
    return pl.pallas_call(
        _attention,
        out_shape=jax.ShapeDtypeStruct((rows, width), BF16),
        in_specs=[here, here, here, anywhere, anywhere, anywhere, anywhere],
        out_specs=here,
        scratch_shapes=[pltpu.VMEM((4, rows, width), BF16), pltpu.VMEM((3, width, columns), BF16), pltpu.VMEM((4, columns, width), BF16),
                        pltpu.VMEM((2, 2, half, HEAD), F32), pltpu.VMEM((heads, tokens, HEAD), BF16), pltpu.VMEM((heads, tokens, HEAD), BF16),
                        pltpu.VMEM((heads, tokens, HEAD), BF16), pltpu.VMEM((heads, rows), F32), pltpu.VMEM((heads, HEAD + 8, rows), F32),
                        pltpu.VMEM((4, rows, columns), BF16), pltpu.VMEM((4, rows, columns), BF16), pltpu.VMEM((2, half, columns), BF16),
                        pltpu.VMEM((rows, width), F32), pltpu.SemaphoreType.DMA((4,)), pltpu.SemaphoreType.DMA((n,)), pltpu.SemaphoreType.DMA((n,))],
        compiler_params=pltpu.CompilerParams(collective_id=0, has_side_effects=True, vmem_limit_bytes=VMEM),
        cost_estimate=pl.CostEstimate(flops=2 * tokens * width * columns * 4, transcendentals=heads * tokens * tokens,
                                      bytes_accessed=8 * width * columns),
        name="attention_half",
    )(x, gain.reshape(1, -1), turn, wq, wk, wv, wo)


def solution(mesh):
    def step(x, gain_a, wq, wk, wv, wo, gain_m, w_gate, w_up, w_down):
        h = attention_half(x, gain_a, wq, wk, wv, wo)
        return mlp_half(h, gain_m, w_gate, w_up, w_down)

    tokens, columns, rows_of = P(("dp", "tp"), None), P(None, "tp"), P("tp", None)
    return jax.shard_map(
        step,
        mesh=mesh,
        in_specs=(tokens, P(None), columns, columns, columns, rows_of, P(None), columns, columns, rows_of),
        out_specs=tokens,
        check_vma=False,
    )
```

```python
import functools

import jax
import jax.numpy as jnp
import numpy as np
from jax import lax
from jax.experimental import pallas as pl
from jax.experimental.pallas import tpu as pltpu
from jax.sharding import PartitionSpec as P

HEAD = 128
THETA = 10000
NEG = -1e30
HIDDEN = 2 * NEG
LOG2E = 1.4426950408889634
VMEM = 67043328
TILE = 512
F32, BF16 = jnp.float32, jnp.bfloat16
OWN, LEFT, RIGHT, OPP = 0, 1, 2, 3


def _dot(a, b, ca=1, cb=0):
    return lax.dot_general(a, b, (((ca,), (cb,)), ((), ())), preferred_element_type=F32)


def _ring():
    n = lax.axis_size("tp")
    me = lax.axis_index("tp")
    return me, lax.rem(me + n - 1, n), lax.rem(me + 1, n), lax.rem(me + 2, n)


def _greet(peers):
    barrier = pltpu.get_barrier_semaphore()
    for peer in peers:
        pl.semaphore_signal(barrier, inc=1, device_id=peer, device_id_type=pl.DeviceIdType.MESH)
    pl.semaphore_wait(barrier, len(peers))


def _norm(src, gain_ref, dst, at, rows, step=32):
    gain = gain_ref[...].astype(F32).reshape(1, -1)

    @pl.loop(0, rows // step)
    def _(i):
        here = pl.ds(pl.multiple_of(at + i * step, step), step)
        wide = src[here, :].astype(F32)
        scale = lax.rsqrt(jnp.mean(wide * wide, -1, keepdims=True) + 1e-6)
        dst[here, :] = (wide * scale * gain).astype(BF16)


class _Copies:
    def __init__(self, send, recv, me):
        self.send, self.recv, self.n, self.all = send, recv, 0, []
        self.peer = lambda s: {"tp": lax.rem(me + 1 + 2 * s, lax.axis_size("tp"))}

    def _make(self, at, src, dst, peer):
        return pltpu.make_async_remote_copy(src_ref=src, dst_ref=dst, send_sem=self.send.at[at], recv_sem=self.recv.at[at], device_id=peer,
                                            device_id_type=pl.DeviceIdType.MESH)

    def one(self, src, dst, peer):
        copy = self._make(self.n, src, dst, peer)
        self.n += 1
        self.all.append(copy)
        return copy

    def sides(self, refs):
        first = self.n
        self.n += 2
        get = lambda s: self._make(first + s, *refs(s), self.peer(s))
        self.all += [get(0), get(1)]
        return get

    def wait_send(self):
        for copy in self.all:
            copy.wait_send()


def _rows(i, n):
    return pl.ds(pl.multiple_of(i * n, n), n)


def _gather(copies, tok, half):
    first = copies.sides(lambda s: (tok.at[OWN, _rows(s, half)], tok.at[1 + s, _rows(s, half)]))
    second = copies.sides(lambda s: (tok.at[OWN, _rows(1 - s, half)], tok.at[1 + s, _rows(1 - s, half)]))
    third = copies.sides(lambda s: (tok.at[1 + s, _rows(s, half)], tok.at[OPP, _rows(s, half)]))
    return first, second, third


def _send_own(src, gain_ref, tok, half, first, second):
    _norm(src, gain_ref, tok.at[OWN], 0, half)
    first(0).start()
    _norm(src, gain_ref, tok.at[OWN], half, half)
    first(1).start()
    second(0).start()
    second(1).start()


MLP_PARTS = 4


def _mlp(h_ref, gain_ref, wg_hbm, wu_hbm, wd_hbm, y_ref, tok, wg, wu, wd, hid, own, mid, dsend, osend, ssend, drecv, orecv, srecv,
         wsem, ssem, rsem):
    me, to_left, to_right, _ = _ring()
    rows, width = h_ref.shape
    half = rows // 2
    part = half // MLP_PARTS
    ff = wg.shape[1]

    def load(i, j):
        hbm, ref = ((wg_hbm, wg), (wu_hbm, wu), (wd_hbm, wd))[i]
        cols = _rows(j, TILE)
        return pltpu.make_async_copy(hbm.at[:, cols], ref.at[:, cols], wsem.at[i, j])

    for j in range(ff // TILE):
        load(0, j).start()
        load(1, j).start()
    for j in range(width // TILE):
        load(2, j).start()
    _greet(({"tp": to_right}, {"tp": to_left}))

    copies = _Copies(ssem, rsem, me)
    first, second, third = _gather(copies, tok, half)
    direct = copies.sides(lambda s: (dsend.at[s], drecv.at[s]))
    opp = [copies.sides(lambda s, p=p: (osend.at[s, _rows(p, part)], orecv.at[s, _rows(p, part)])) for p in range(MLP_PARTS)]
    total = [copies.sides(lambda s, p=p: (ssend.at[s, _rows(p, part)], srecv.at[s, _rows(p, part)])) for p in range(MLP_PARTS)]
    _send_own(h_ref, gain_ref, tok, half, first, second)

    def term(slot, i, store, fresh=None):
        here = _rows(i, half)

        def arrived(n, j):
            if fresh is not None:
                pl.when(fresh)(lambda: load(n, j).wait())

        @pl.loop(0, ff // TILE)
        def _(j):
            cols = _rows(j, TILE)
            arrived(0, j)
            arrived(1, j)
            gate = _dot(tok[slot, here, :], wg[:, cols])
            up = _dot(tok[slot, here, :], wu[:, cols])
            hid[:, cols] = (jax.nn.silu(gate) * up).astype(BF16)

        @pl.loop(0, width // TILE)
        def _(j):
            cols = _rows(j, TILE)
            arrived(2, j)
            store(cols, _dot(hid[...], wd[:, cols]))

    def put(ref, side):
        def store(cols, t):
            ref[side, :, cols] = t.astype(ref.dtype)

        return store

    @pl.loop(0, 2)
    def _(i):
        def store(cols, t):
            here = _rows(i, half)
            own[here, cols] = h_ref[here, cols].astype(F32) + t

        term(OWN, i, store, fresh=i == 0)

    for s in (0, 1):
        first(s).wait_recv()
        third(s).start()

    @pl.loop(0, 2)
    def _(s):
        term(2 - s, 1 - s, put(dsend, s))
        direct(s).start()

    @pl.loop(0, 2)
    def _(s):
        second(1 - s).wait_recv()
        term(2 - s, s, put(mid, s))

    @pl.loop(0, 2)
    def _(s):
        third(s).wait_recv()
        term(OPP, s, put(osend, s))
        for c in opp:
            c(s).start()

    for p in range(MLP_PARTS):
        here = _rows(p, part)
        for s in (0, 1):
            opp[p](s).wait_recv()
            ssend[s, here] = (mid[s, here] + orecv[s, here].astype(F32)).astype(BF16)
            total[p](s).start()
    for s in (0, 1):
        direct(s).wait_recv()
    for p in range(MLP_PARTS):
        there = _rows(p, part)
        for s in (0, 1):
            total[p](s).wait_recv()
            here = pl.ds(s * half + p * part, part)
            y_ref[here, :] = (own[here, :] + srecv[s, there].astype(F32) + drecv[1 - s, there].astype(F32)).astype(BF16)
    copies.wait_send()


def mlp_half(h, gain, w_gate, w_up, w_down):
    rows, width = h.shape
    ff = w_gate.shape[1]
    half = rows // 2
    n = 8 + 4 * MLP_PARTS
    anywhere, here = pl.BlockSpec(memory_space=pl.ANY), pl.BlockSpec(memory_space=pltpu.VMEM)
    halves = lambda kind: pltpu.VMEM((2, half, width), kind)
    return pl.pallas_call(
        _mlp,
        out_shape=jax.ShapeDtypeStruct((rows, width), BF16),
        in_specs=[here, here, anywhere, anywhere, anywhere],
        out_specs=here,
        scratch_shapes=[pltpu.VMEM((4, rows, width), BF16), pltpu.VMEM((width, ff), BF16), pltpu.VMEM((width, ff), BF16),
                        pltpu.VMEM((ff, width), BF16), pltpu.VMEM((half, ff), BF16), pltpu.VMEM((rows, width), F32), halves(F32),
                        halves(BF16), halves(BF16), halves(BF16), halves(BF16), halves(BF16), halves(BF16),
                        pltpu.SemaphoreType.DMA((3, max(ff, width) // TILE)), pltpu.SemaphoreType.DMA((n,)), pltpu.SemaphoreType.DMA((n,))],
        compiler_params=pltpu.CompilerParams(collective_id=1, has_side_effects=True, vmem_limit_bytes=VMEM),
        cost_estimate=pl.CostEstimate(flops=24 * rows * width * ff, transcendentals=4 * rows * ff, bytes_accessed=6 * width * ff),
        name="mlp_half",
    )(h, gain, w_gate, w_up, w_down)


def _attention(x_ref, gain_ref, turn_ref, wq_hbm, wk_hbm, wv_hbm, wo_hbm, h_ref, tok, w, wo, table, q, k, v, top_s, mix_s, out, got, relay, acc,
               wsem, ssem, rsem):
    me, to_left, to_right, to_opp = _ring()
    n = lax.axis_size("tp")
    dp = lax.axis_index("dp")
    core, side = lax.rem(dp, 2), lax.rem(lax.div(dp, 2), 2)
    core_peer, chip_peer = {"dp": dp + 1 - 2 * core}, {"dp": dp + 2 - 4 * side}
    rows, width = x_ref.shape
    half = rows // 2
    heads = q.shape[0]

    def block_of(slot):
        return lax.rem(me + (0, n - 1, 1, 2)[slot], n) if isinstance(slot, int) else lax.rem(me + n + 2 * slot - 3, n)

    loads = [pltpu.make_async_copy(hbm, w.at[i], wsem.at[i]) for i, hbm in enumerate((wq_hbm, wk_hbm, wv_hbm))]
    loads.append(pltpu.make_async_copy(wo_hbm, wo.at[OWN], wsem.at[3]))
    for c in loads:
        c.start()

    copies = _Copies(ssem, rsem, me)
    first, second, third = _gather(copies, tok, half)
    eighth = wo.shape[1] // 8
    mine = lambda c: _rows(4 * side + 2 * core + c, eighth)
    beside = lambda c: _rows(4 * (1 - side) + 2 * core + c, eighth)
    wo_x = [copies.sides(lambda s, c=c: ((wo_hbm.at[mine(c)] if c == 0 else wo.at[OWN, mine(c)]), wo.at[1 + s, mine(c)])) for c in (0, 1)]
    wo_f = copies.sides(lambda s: (wo.at[1 + s, mine(s)], wo.at[OPP, mine(s)]))
    slots = (LEFT, RIGHT, OPP)
    wo_z = {(t, c): copies.one(wo.at[t, mine(c)], wo.at[t, mine(c)], chip_peer) for c in (0, 1) for t in slots}
    wo_d = {(t, c): copies.one(wo.at[t, mine(c)], wo.at[t, mine(c)], core_peer) for c in (0, 1) for t in slots}
    wo_e = {(t, c): copies.one(wo.at[t, beside(c)], wo.at[t, beside(c)], core_peer) for c in (0, 1) for t in slots}

    _greet(({"tp": to_right}, {"tp": to_left}, core_peer, chip_peer))
    wo_x[0](0).start()
    wo_x[0](1).start()
    _send_own(x_ref, gain_ref, tok, half, first, second)

    def spread(t, c):
        wo_z[t, c].start()
        wo_d[t, c].start()

    def spread_on(t, c):
        wo_z[t, c].wait_recv()
        wo_e[t, c].start()

    def angles(block, i, t):
        place = lax.broadcasted_iota(jnp.int32, (half, HEAD), 0) + (block * rows + i * half)
        angle = place.astype(F32) * turn_ref[...]
        sign = jnp.where(lax.broadcasted_iota(jnp.int32, (half, HEAD), 1) < HEAD // 2, -1.0, 1.0)
        table[t, 0] = jnp.cos(angle)
        table[t, 1] = jnp.sin(angle) * sign

    def project(slot, block, i, t, fresh=None):
        here = _rows(i, half)
        there = _rows(2 * block + i, half)
        for m, ref in enumerate((q, k, v)):
            if fresh is not None:
                pl.when(fresh)(lambda: loads[m].wait())
            full = _dot(tok[slot, here, :], w[m]).astype(BF16)
            for a in range(heads):
                one = full[:, a * HEAD : (a + 1) * HEAD]
                if m < 2:
                    wide = one.astype(F32)
                    ref[a, there, :] = (wide * table[t, 0] + pltpu.roll(wide, HEAD // 2, 1) * table[t, 1]).astype(BF16)
                else:
                    ref[a, :HEAD, there] = one.T

    e = HEAD**-0.5 * LOG2E

    def unit(bq, bk, masked):
        mine, here = _rows(bq, rows), _rows(bk, rows)
        scores = [_dot(k[a, here, :], q[a, mine, :], 1, 1) for a in range(heads)]
        weights, keeps = [], []
        for a, s in enumerate(scores):
            if masked:
                s = jnp.where(lax.broadcasted_iota(jnp.int32, s.shape, 1) >= lax.broadcasted_iota(jnp.int32, s.shape, 0), s, HIDDEN)
            old = top_s[bq, a : a + 1, :]
            top = jnp.maximum(old, s.max(axis=0, keepdims=True))
            top_s[bq, a : a + 1, :] = top
            weights.append(jnp.exp2((s - top) * e).astype(BF16))
            keeps.append(jnp.exp2((old - top) * e))
        for a, (p, keep) in enumerate(zip(weights, keeps)):
            mix_s[bq, a] = mix_s[bq, a] * keep + _dot(v[a, :, here], p)

    def pair(a, b):
        unit(jnp.maximum(a, b), jnp.minimum(a, b), False)

    @pl.loop(0, n)
    def _(b):
        top_s[b] = jnp.full(top_s.shape[1:], NEG, F32)
        mix_s[b] = jnp.zeros(mix_s.shape[1:], F32)

    for a in range(heads):
        v[a, HEAD:, :] = jnp.ones((v.shape[1] - HEAD, v.shape[2]), BF16)

    @pl.loop(0, 2)
    def _(i):
        angles(me, i, 0)
        project(OWN, me, i, 0, fresh=i == 0)

    for s in (0, 1):
        wo_x[0](s).wait_recv()
        spread(1 + s, 0)
    unit(me, me, True)

    @pl.loop(0, 2)
    def _(s):
        angles(block_of(2 - s), 1 - s, s)

    for s in (0, 1):
        first(s).wait_recv()
        third(s).start()

    @pl.loop(0, 2)
    def _(s):
        project(2 - s, block_of(2 - s), 1 - s, s)
        angles(block_of(2 - s), s, s)

    @pl.loop(0, 2)
    def _(s):
        second(1 - s).wait_recv()
        project(2 - s, block_of(2 - s), s, s)
        angles(to_opp, s, s)
        unit(block_of(2 - s), block_of(2 - s), True)

    @pl.loop(0, 3)
    def _(i):
        pair(lax.rem(me + n - lax.div(i, 2), n), lax.rem(me + n - 1 + 2 * jnp.minimum(i, 1), n))

    for s in (0, 1):
        spread_on(1 + s, 0)
    loads[3].wait()
    for s in (0, 1):
        third(s).wait_recv()
        wo_x[1](s).start()
    wo_f(0).start()

    @pl.loop(0, 2)
    def _(s):
        project(OPP, to_opp, s, s)

    for s in (0, 1):
        wo_x[1](s).wait_recv()
        spread(1 + s, 1)
    wo_f(1).start()
    unit(to_opp, to_opp, True)

    @pl.loop(0, 3)
    def _(i):
        pair(to_opp, lax.rem(me + n - 1 + i, n))

    wo_f(0).wait_recv()
    spread(OPP, 0)

    def finish(slot):
        block = block_of(slot)
        for a in range(heads):
            out[slot, :, a * HEAD : (a + 1) * HEAD] = (mix_s[block, a, :HEAD, :] * (1 / mix_s[block, a, HEAD : HEAD + 1, :])).T.astype(BF16)

    out_o = copies.sides(lambda s: (out.at[OPP, _rows(s, half)], relay.at[s]))
    out_n = copies.sides(lambda s: (out.at[2 - s], got.at[1 + s]))
    out_f = copies.sides(lambda s: (relay.at[s], got.at[OPP, _rows(s, half)]))
    finish(OPP)
    for s in (0, 1):
        out_o(s).start()
    for s in (0, 1):
        finish(2 - s)
        out_n(s).start()
    finish(OWN)
    wo_f(1).wait_recv()
    spread(OPP, 1)
    for s in (0, 1):
        out_o(s).wait_recv()
        out_f(s).start()
    spread_on(LEFT, 1)
    spread_on(RIGHT, 1)

    @pl.loop(0, width // TILE)
    def _(j):
        cols = _rows(j, TILE)
        acc[:, cols] = x_ref[:, cols].astype(F32) + _dot(out[OWN], wo[OWN, :, cols])

    spread_on(OPP, 0)
    for t in (LEFT, RIGHT):
        for c in (0, 1):
            wo_d[t, c].wait_recv()
            wo_e[t, c].wait_recv()
    for s in (0, 1):
        out_n(s).wait_recv()

    @pl.loop(0, width // TILE)
    def _(j):
        cols = _rows(j, TILE)
        acc[:, cols] += _dot(got[LEFT], wo[LEFT, :, cols]) + _dot(got[RIGHT], wo[RIGHT, :, cols])

    spread_on(OPP, 1)
    for c in (0, 1):
        wo_d[OPP, c].wait_recv()
        wo_e[OPP, c].wait_recv()
    for s in (0, 1):
        out_f(s).wait_recv()

    @pl.loop(0, width // TILE)
    def _(j):
        cols = _rows(j, TILE)
        h_ref[:, cols] = (acc[:, cols] + _dot(got[OPP], wo[OPP, :, cols])).astype(BF16)

    copies.wait_send()


def attention_half(x, gain, wq, wk, wv, wo):
    rows, width = x.shape
    columns = wq.shape[1]
    heads, half = columns // HEAD, rows // 2
    n = 36
    anywhere, here = pl.BlockSpec(memory_space=pl.ANY), pl.BlockSpec(memory_space=pltpu.VMEM)
    low = HEAD // 2
    turn = np.float32(THETA) ** (-np.arange(low, dtype=np.float32) / np.float32(low))
    turn = jnp.asarray(np.tile(turn, 2)[None])
    tokens = 4 * rows
    return pl.pallas_call(
        _attention,
        out_shape=jax.ShapeDtypeStruct((rows, width), BF16),
        in_specs=[here, here, here, anywhere, anywhere, anywhere, anywhere],
        out_specs=here,
        scratch_shapes=[pltpu.VMEM((4, rows, width), BF16), pltpu.VMEM((3, width, columns), BF16), pltpu.VMEM((4, columns, width), BF16),
                        pltpu.VMEM((2, 2, half, HEAD), F32), pltpu.VMEM((heads, tokens, HEAD), BF16), pltpu.VMEM((heads, tokens, HEAD), BF16),
                        pltpu.VMEM((heads, HEAD + 16, tokens), BF16), pltpu.VMEM((4, heads, rows), F32), pltpu.VMEM((4, heads, HEAD + 16, rows), F32),
                        pltpu.VMEM((4, rows, columns), BF16), pltpu.VMEM((4, rows, columns), BF16), pltpu.VMEM((2, half, columns), BF16),
                        pltpu.VMEM((rows, width), F32), pltpu.SemaphoreType.DMA((4,)), pltpu.SemaphoreType.DMA((n,)), pltpu.SemaphoreType.DMA((n,))],
        compiler_params=pltpu.CompilerParams(collective_id=0, has_side_effects=True, vmem_limit_bytes=VMEM),
        cost_estimate=pl.CostEstimate(flops=2 * tokens * width * columns * 4, transcendentals=heads * tokens * tokens,
                                      bytes_accessed=8 * width * columns),
        name="attention_half",
    )(x, gain, turn, wq, wk, wv, wo)


def solution(mesh):
    def step(x, gain_a, wq, wk, wv, wo, gain_m, w_gate, w_up, w_down):
        h = attention_half(x, gain_a, wq, wk, wv, wo)
        return mlp_half(h, gain_m, w_gate, w_up, w_down)

    tokens, columns, rows_of = P(("dp", "tp"), None), P(None, "tp"), P("tp", None)
    return jax.shard_map(
        step,
        mesh=mesh,
        in_specs=(tokens, P(None), columns, columns, columns, rows_of, P(None), columns, columns, rows_of),
        out_specs=tokens,
        check_vma=False,
    )
```

```python
import jax
import jax.numpy as jnp
import numpy as np
from jax import lax
from jax.experimental import pallas as pl
from jax.experimental.pallas import tpu as pltpu
from jax.sharding import PartitionSpec as P

HEAD = 128
THETA = 10000
NEG = -1e30
HIDDEN = 2 * NEG
LOG2E = 1.4426950408889634
VMEM = 67043328 - 2 * 2**20 - 2**18
TILE = 512
F32, BF16 = jnp.float32, jnp.bfloat16
OWN, LEFT, RIGHT, OPP = 0, 1, 2, 3


def _dot(a, b, ca=1, cb=0):
    return lax.dot_general(a, b, (((ca,), (cb,)), ((), ())), preferred_element_type=F32)


def _greet(peers):
    barrier = pltpu.get_barrier_semaphore()
    for peer in peers:
        pl.semaphore_signal(barrier, inc=1, device_id=peer, device_id_type=pl.DeviceIdType.MESH)
    pl.semaphore_wait(barrier, len(peers))


def _norm(src, gain_ref, dst, step=32):
    gain = gain_ref[...].astype(F32).reshape(1, -1)

    @pl.loop(0, src.shape[0] // step)
    def _(i):
        wide = src[_rows(i, step), :].astype(F32)
        scale = lax.rsqrt(jnp.mean(wide * wide, -1, keepdims=True) + 1e-6)
        dst[_rows(i, step), :] = (wide * scale * gain).astype(BF16)


class _Started:
    def __init__(self, copies):
        self.copies = copies

    def wait_send(self):
        for copy in self.copies:
            copy.wait_send()


class _Copies:
    def __init__(self, send, recv, me):
        self.send, self.recv, self.n, self.all = send, recv, 0, []
        self.peer = lambda s: {"tp": lax.rem(me + 1 + 2 * s, lax.axis_size("tp"))}

    def _make(self, at, src, dst, peer):
        return pltpu.make_async_remote_copy(src_ref=src, dst_ref=dst, send_sem=self.send.at[at], recv_sem=self.recv.at[at], device_id=peer,
                                            device_id_type=pl.DeviceIdType.MESH)

    def one(self, src, dst, peer):
        copy = self._make(self.n, src, dst, peer)
        self.n += 1
        self.all.append(copy)
        return copy

    def sides(self, refs):
        first = self.n
        self.n += 2
        get = lambda s: self._make(first + s, *refs(s), self.peer(s))
        self.all += [get(0), get(1)]
        return get

    def take(self):
        taken, self.all = _Started(self.all), []
        return taken


def _rows(i, n):
    return pl.ds(pl.multiple_of(i * n, n), n)


PARTS = 4


def _layer(x_hbm, gain_a_ref, gain_m_ref, turn_ref, wq_hbm, wk_hbm, wv_hbm, wo_hbm, wg_hbm, wu_hbm, wd_hbm, y_ref, tok, bg, bu, bd, bo, ssend, orecv,
           state, top_s, acc, hid, table, wsem, lsem, ssem, rsem):
    n = lax.axis_size("tp")
    me = lax.axis_index("tp")
    dp = lax.axis_index("dp")
    core, side = lax.rem(dp, 2), lax.rem(lax.div(dp, 2), 2)
    core_peer, chip_peer = {"dp": dp + 1 - 2 * core}, {"dp": dp + 2 - 4 * side}
    rows, width = x_hbm.shape
    half, quarter, part = rows // 2, rows // 4, rows // 2 // PARTS
    ff = bg.shape[1]
    columns = wq_hbm.shape[1]
    heads = columns // HEAD
    deep = HEAD + 16
    sides, tiles = (0, 1), width // TILE
    to_opp = lax.rem(me + 2, n)

    def block_of(slot):
        return lax.rem(me + (0, n - 1, 1, 2)[slot], n) if isinstance(slot, int) else lax.rem(me + n + 2 * slot - 3, n)

    w = lambda m: bg.at[:, pl.ds(m * columns, columns)]
    head = lambda ref, a: ref.at[:, a * HEAD : (a + 1) * HEAD]
    q = lambda a: bu.at[:, pl.ds(a * HEAD, HEAD)]
    k = lambda a: bu.at[:, pl.ds(columns + a * HEAD, HEAD)]
    v = lambda a: bd.at[pl.ds(a * deep, deep), :]
    low = ff - 2 * rows
    relay = lambda s: bd.at[pl.ds(low - half, half), _rows(s, columns)]
    out = lambda slot: bd.at[pl.ds(low, rows), _rows(slot, columns)]
    got = lambda slot: bd.at[pl.ds(low + rows, rows), _rows(slot, columns)]
    wo = bo
    mix = lambda bq, a: state.at[_rows(bq * heads + a, deep), :]
    halved = lambda slot: (lambda s, at=None: bo.at[slot, _rows(s, half) if at is None else _rows(s * PARTS + at, part)])
    drecv, srecv, dsend, osend = halved(0), halved(1), halved(2), halved(3)
    mid = lambda s, j: state.at[_rows(s * tiles + j, half), :]

    x = ssend
    takes = [pltpu.make_async_copy(x_hbm.at[_rows(i, half)], x.at[i], wsem.at[4 + i]) for i in (0, 1)]
    for take in takes:
        take.start()
    loads = [pltpu.make_async_copy(hbm, w(m), wsem.at[m]) for m, hbm in enumerate((wq_hbm, wk_hbm, wv_hbm))]
    loads.append(pltpu.make_async_copy(wo_hbm, wo.at[OWN], wsem.at[3]))
    for load in loads:
        load.start()

    def load(m, j):
        hbm, ref = ((wg_hbm, bg), (wu_hbm, bu), (wd_hbm, bd))[m]
        return pltpu.make_async_copy(hbm.at[:, _rows(j, TILE)], ref.at[:, _rows(j, TILE)], lsem.at[m, j])

    copies = _Copies(ssem, rsem, me)

    def own_rows(at, size):
        return lambda s: (tok.at[OWN, _rows(at(s), size)], tok.at[1 + s, _rows(at(s), size)])

    forward = lambda s: (tok.at[1 + s, _rows(s, half)], tok.at[OPP, _rows(s, half)])
    first = copies.sides(own_rows(lambda s: s, half))
    second = copies.sides(own_rows(lambda s: 1 - s, half))
    third = copies.sides(forward)
    gathered = copies.take()

    eighth = rows // 8
    mine = lambda c: _rows(4 * side + 2 * core + c, eighth)
    beside = lambda c: _rows(4 * (1 - side) + 2 * core + c, eighth)
    wo_early = copies.sides(lambda s: (wo_hbm.at[mine(s)], wo.at[1 + s, mine(s)]))
    wo_late = copies.sides(lambda s: (wo.at[OWN, mine(1 - s)], wo.at[1 + s, mine(1 - s)]))
    wo_third = copies.sides(lambda s: (wo.at[1 + s, mine(s)], wo.at[OPP, mine(s)]))
    pieces = [(t, c) for t in (LEFT, RIGHT, OPP) for c in (0, 1)]
    wo_chip = {(t, c): copies.one(wo.at[t, mine(c)], wo.at[t, mine(c)], chip_peer) for t, c in pieces}
    wo_core = {(t, c): copies.one(wo.at[t, mine(c)], wo.at[t, mine(c)], core_peer) for t, c in pieces}
    wo_both = {(t, c): copies.one(wo.at[t, beside(c)], wo.at[t, beside(c)], core_peer) for t, c in pieces}
    fetched = copies.take()

    def spread(t, c):
        wo_chip[t, c].start()
        wo_core[t, c].start()

    def spread_on(t, c):
        wo_chip[t, c].wait_recv()
        wo_both[t, c].start()

    def complete(t):
        for c in (0, 1):
            wo_core[t, c].wait_recv()
            wo_both[t, c].wait_recv()

    at = lambda i, p: _rows(2 * i + p, quarter)
    out_o = [copies.sides(lambda s, p=p: (out(OPP).at[at(s, p)], relay(s).at[_rows(p, quarter)])) for p in (0, 1)]
    out_n = [[copies.sides(lambda s, p=p, i=i: (out(2 - s).at[at(i, p)], got(1 + s).at[at(i, p)])) for i in (0, 1)] for p in (0, 1)]
    out_f = [copies.sides(lambda s, p=p: (relay(s).at[_rows(p, quarter)], got(OPP).at[at(s, p)])) for p in (0, 1)]
    exchanged = copies.take()

    first_m = [copies.sides(own_rows(lambda s, p=p: 2 * s + p, quarter)) for p in (0, 1)]
    second_m = copies.sides(own_rows(lambda s: 1 - s, half))
    third_m = copies.sides(forward)
    direct = copies.sides(lambda s: (dsend(s), drecv(s)))
    opp = [copies.sides(lambda s, p=p: (osend(s, p), orecv.at[s, _rows(p, part)])) for p in range(PARTS)]
    total = [copies.sides(lambda s, p=p: (ssend.at[s, _rows(p, part)], srecv(s, p))) for p in range(PARTS)]
    last = copies.take()

    _greet(({"tp": lax.rem(me + 1, n)}, {"tp": lax.rem(me + n - 1, n)}, core_peer, chip_peer))
    for s in sides:
        wo_early(s).start()
    for s in sides:
        takes[s].wait()
        _norm(x.at[s], gain_a_ref, tok.at[OWN, _rows(s, half)])
        first(s).start()
    for s in sides:
        second(s).start()

    def angles(block, i, t):
        place = lax.broadcasted_iota(jnp.int32, (half, HEAD), 0) + (block * rows + i * half)
        angle = place.astype(F32) * turn_ref[...]
        sign = jnp.where(lax.broadcasted_iota(jnp.int32, (half, HEAD), 1) < HEAD // 2, -1.0, 1.0)
        table[t, 0] = jnp.cos(angle)
        table[t, 1] = jnp.sin(angle) * sign

    def project(slot, block, i, t, fresh=None):
        here = _rows(i, half)
        there = _rows(2 * block + i, half)
        for m in range(3):
            if fresh is not None:
                pl.when(fresh)(lambda: loads[m].wait())
            full = _dot(tok[slot, here, :], w(m)[...]).astype(BF16)
            for a in range(heads):
                one = full[:, a * HEAD : (a + 1) * HEAD]
                if m < 2:
                    wide = one.astype(F32)
                    (q, k)[m](a)[there, :] = (wide * table[t, 0] + pltpu.roll(wide, HEAD // 2, 1) * table[t, 1]).astype(BF16)
                else:
                    v(a)[:HEAD, there] = one.T

    e = HEAD**-0.5 * LOG2E

    def unit(bq, bk, masked):
        mine, here = _rows(bq, rows), _rows(bk, rows)
        scores = [_dot(k(a)[here, :], q(a)[mine, :], 1, 1) for a in range(heads)]
        weights, keeps = [], []
        for a, s in enumerate(scores):
            if masked:
                s = jnp.where(lax.broadcasted_iota(jnp.int32, s.shape, 1) >= lax.broadcasted_iota(jnp.int32, s.shape, 0), s, HIDDEN)
            old = top_s[bq, a : a + 1, :]
            top = jnp.maximum(old, s.max(axis=0, keepdims=True))
            top_s[bq, a : a + 1, :] = top
            weights.append(jnp.exp2((s - top) * e).astype(BF16))
            keeps.append(jnp.exp2((old - top) * e))
        for a, (p, keep) in enumerate(zip(weights, keeps)):
            mix(bq, a)[...] = mix(bq, a)[...] * keep + _dot(v(a)[:, here], p)

    def pair(a, b):
        unit(jnp.maximum(a, b), jnp.minimum(a, b), False)

    def finish(slot):
        block = block_of(slot)
        for a in range(heads):
            got_it = mix(block, a)[:HEAD, :] * (1 / mix(block, a)[HEAD : HEAD + 1, :])
            head(out(slot), a)[...] = got_it.T.astype(BF16)

    @pl.loop(0, n)
    def _(b):
        top_s[b] = jnp.full(top_s.shape[1:], NEG, F32)
        for a in range(heads):
            mix(b, a)[...] = jnp.zeros((deep, rows), F32)

    for a in range(heads):
        v(a)[HEAD:, :] = jnp.ones((deep - HEAD, width), BF16)

    @pl.loop(0, 2)
    def _(i):
        angles(me, i, 0)
        project(OWN, me, i, 0, fresh=i == 0)

    for s in sides:
        wo_early(s).wait_recv()
        spread(1 + s, s)
    unit(me, me, True)

    @pl.loop(0, 2)
    def _(s):
        angles(block_of(2 - s), 1 - s, s)

    for s in sides:
        first(s).wait_recv()
        third(s).start()

    @pl.loop(0, 2)
    def _(s):
        project(2 - s, block_of(2 - s), 1 - s, s)
        angles(block_of(2 - s), s, s)

    @pl.loop(0, 2)
    def _(s):
        second(1 - s).wait_recv()
        project(2 - s, block_of(2 - s), s, s)
        angles(to_opp, s, s)
        unit(block_of(2 - s), block_of(2 - s), True)

    @pl.loop(0, 3)
    def _(i):
        pair(lax.rem(me + n - lax.div(i, 2), n), lax.rem(me + n - 1 + 2 * jnp.minimum(i, 1), n))

    for s in sides:
        spread_on(1 + s, s)
    loads[3].wait()
    for s in sides:
        third(s).wait_recv()
        wo_late(s).start()
        wo_third(s).start()

    @pl.loop(0, 2)
    def _(s):
        project(OPP, to_opp, s, s)

    for j in range(ff // TILE):
        load(0, j).start()
    unit(to_opp, to_opp, True)

    @pl.loop(0, 3)
    def _(i):
        pair(to_opp, lax.rem(me + n - 1 + i, n))

        @pl.when(i == 1)
        def _():
            for s in sides:
                wo_late(s).wait_recv()
                spread(1 + s, 1 - s)

    for j in range(ff // TILE):
        load(1, j).start()
    gathered.wait_send()
    finish(OPP)
    for s in sides:
        out_o[0](s).start()
    for s in sides:
        finish(2 - s)
        for i in (0, 1):
            out_n[0][i](s).start()
    for s in sides:
        out_o[1](s).start()
    finish(OWN)
    for s in sides:
        wo_third(s).wait_recv()
        spread(OPP, s)
    for s in sides:
        out_o[0](s).wait_recv()
        out_f[0](s).start()
        for i in (0, 1):
            out_n[1][i](s).start()

    def lhs(ref, p):
        return jnp.concatenate([ref[at(i, p), :] for i in (0, 1)], axis=0)

    def most(p):
        for i in (0, 1):
            for s in sides:
                out_n[p][i](s).wait_recv()

        @pl.loop(0, tiles)
        def _(j):
            cols = _rows(j, TILE)
            t = _dot(lhs(out(OWN), p), wo[OWN, :, cols]) + _dot(lhs(got(LEFT), p), wo[LEFT, :, cols]) + _dot(lhs(got(RIGHT), p), wo[RIGHT, :, cols])
            for i in (0, 1):
                acc[at(i, p), cols] = x[i, _rows(p, quarter), cols].astype(F32) + t[i * quarter : (i + 1) * quarter]

    def rest(p):
        for s in sides:
            out_f[p](s).wait_recv()

        @pl.loop(0, tiles)
        def _(j):
            cols = _rows(j, TILE)
            t = _dot(lhs(got(OPP), p), wo[OPP, :, cols])
            for i in (0, 1):
                acc[at(i, p), cols] = (acc[at(i, p), cols] + t[i * quarter : (i + 1) * quarter]).astype(BF16).astype(F32)

        for i in (0, 1):
            _norm(acc.at[at(i, p)], gain_m_ref, tok.at[OWN, at(i, p)])
            first_m[p](i).start()

    for s in sides:
        spread_on(1 + s, 1 - s)
    for t in (LEFT, RIGHT):
        complete(t)
    most(0)
    for s in sides:
        out_o[1](s).wait_recv()
        out_f[1](s).start()
    for c in (0, 1):
        spread_on(OPP, c)
    complete(OPP)
    rest(0)
    fetched.wait_send()
    most(1)
    rest(1)
    for s in sides:
        second_m(s).start()
    exchanged.wait_send()
    for j in range(width // TILE):
        load(2, j).start()

    def term(slot, i, store, fresh=None):
        here = _rows(i, half)

        def arrived(m, j):
            if fresh is not None:
                pl.when(fresh)(lambda: load(m, j).wait())

        @pl.loop(0, ff // TILE)
        def _(j):
            cols = _rows(j, TILE)
            arrived(0, j)
            arrived(1, j)
            gate = _dot(tok[slot, here, :], bg[:, cols])
            up = _dot(tok[slot, here, :], bu[:, cols])
            hid[:, cols] = (jax.nn.silu(gate) * up).astype(BF16)

        @pl.loop(0, tiles)
        def _(j):
            arrived(2, j)
            store(j, _dot(hid[...], bd[:, _rows(j, TILE)]))

    def put(ref):
        def store(j, t):
            ref[:, _rows(j, TILE)] = t.astype(ref.dtype)

        return store

    @pl.loop(0, 2)
    def _(i):
        def store(j, t):
            acc[_rows(i, half), _rows(j, TILE)] += t

        term(OWN, i, store, fresh=i == 0)

    for s in sides:
        for p in (0, 1):
            first_m[p](s).wait_recv()
        third_m(s).start()

    @pl.loop(0, 2)
    def _(s):
        term(2 - s, 1 - s, put(dsend(s)))
        direct(s).start()

    @pl.loop(0, 2)
    def _(s):
        def store(j, t):
            mid(s, j)[...] = t

        second_m(1 - s).wait_recv()
        term(2 - s, s, store)

    @pl.loop(0, 2)
    def _(s):
        third_m(s).wait_recv()
        term(OPP, s, put(osend(s)))
        for c in opp:
            c(s).start()

    for p in range(PARTS):
        here = _rows(p, part)
        for s in sides:
            opp[p](s).wait_recv()
            for j in range(tiles):
                cols = _rows(j, TILE)
                ssend[s, here, cols] = (mid(s, j)[here, :] + orecv[s, here, cols].astype(F32)).astype(BF16)
            total[p](s).start()
    for s in sides:
        direct(s).wait_recv()
    for p in range(PARTS):
        for s in sides:
            total[p](s).wait_recv()
            here = pl.ds(s * half + p * part, part)
            y_ref[here, :] = (acc[here, :] + srecv(s, p)[...].astype(F32) + drecv(1 - s, p)[...].astype(F32)).astype(BF16)
    last.wait_send()


def layer(x, gain_a, wq, wk, wv, wo, gain_m, w_gate, w_up, w_down):
    rows, width = x.shape
    columns, ff = wq.shape[1], w_gate.shape[1]
    heads, half = columns // HEAD, rows // 2
    tokens = 4 * rows
    if not tokens == width == ff == 4 * columns:
        raise ValueError("sizes")
    n = 54 + 2 + 4 * PARTS
    anywhere, here = pl.BlockSpec(memory_space=pl.ANY), pl.BlockSpec(memory_space=pltpu.VMEM)
    low = HEAD // 2
    turn = np.float32(THETA) ** (-np.arange(low, dtype=np.float32) / np.float32(low))
    turn = jnp.asarray(np.tile(turn, 2)[None])
    whole = lambda *shape: pltpu.VMEM(shape, BF16)
    return pl.pallas_call(
        _layer,
        out_shape=pltpu.VMEM((rows, width), BF16),
        in_specs=[anywhere] + [here] * 3 + [anywhere] * 7,
        out_specs=here,
        scratch_shapes=[whole(4, rows, width), whole(width, ff), whole(width, ff), whole(ff, width), whole(4, columns, width),
                        whole(2, half, width), whole(2, half, width), pltpu.VMEM((4 * heads * (HEAD + 16), rows), F32),
                        pltpu.VMEM((4, heads, rows), F32), pltpu.VMEM((rows, width), F32), whole(half, ff), pltpu.VMEM((2, 2, half, HEAD), F32),
                        pltpu.SemaphoreType.DMA((6,)), pltpu.SemaphoreType.DMA((3, ff // TILE)), pltpu.SemaphoreType.DMA((n,)),
                        pltpu.SemaphoreType.DMA((n,))],
        compiler_params=pltpu.CompilerParams(collective_id=0, has_side_effects=True, vmem_limit_bytes=VMEM),
        cost_estimate=pl.CostEstimate(flops=8 * tokens * width * columns + 6 * tokens * width * ff, transcendentals=heads * tokens * tokens,
                                      bytes_accessed=8 * width * columns + 6 * width * ff),
        name="layer",
    )(x, gain_a, gain_m, turn, wq, wk, wv, wo, w_gate, w_up, w_down)


def solution(mesh):
    def step(x, gain_a, wq, wk, wv, wo, gain_m, w_gate, w_up, w_down):
        return layer(x, gain_a, wq, wk, wv, wo, gain_m, w_gate, w_up, w_down)

    tokens, columns, rows_of = P(("dp", "tp"), None), P(None, "tp"), P("tp", None)
    return jax.shard_map(
        step,
        mesh=mesh,
        in_specs=(tokens, P(None), columns, columns, columns, rows_of, P(None), columns, columns, rows_of),
        out_specs=tokens,
        check_vma=False,
    )
```

```python
import functools

import jax
import jax.numpy as jnp
import numpy as np
from jax import lax
from jax.experimental import pallas as pl
from jax.experimental.pallas import tpu as pltpu
from jax.sharding import PartitionSpec as P

HEAD = 128
THETA = 10000
NEG = -1e30
HIDDEN = 2 * NEG
LOG2E = 1.4426950408889634
VMEM = 67043328 - 2 * 2**20 - 2**18
TILE = 512
F32, BF16 = jnp.float32, jnp.bfloat16
OWN, LEFT, RIGHT, OPP = 0, 1, 2, 3


def _dot(a, b, ca=1, cb=0):
    return lax.dot_general(a, b, (((ca,), (cb,)), ((), ())), preferred_element_type=F32)


def _greet(peers):
    barrier = pltpu.get_barrier_semaphore()
    for peer in peers:
        pl.semaphore_signal(barrier, inc=1, device_id=peer, device_id_type=pl.DeviceIdType.MESH)
    pl.semaphore_wait(barrier, len(peers))


def _norm(src, gain_ref, dst, step=32):
    gain = gain_ref[...].astype(F32).reshape(1, -1)

    @pl.loop(0, src.shape[0] // step)
    def _(i):
        wide = src[_rows(i, step), :].astype(F32)
        scale = lax.rsqrt(jnp.mean(wide * wide, -1, keepdims=True) + 1e-6)
        dst[_rows(i, step), :] = (wide * scale * gain).astype(BF16)


class _Started:
    def __init__(self, copies):
        self.copies = copies

    def wait_send(self):
        for copy in self.copies:
            copy.wait_send()


class _Copies:
    def __init__(self, send, recv, me):
        self.send, self.recv, self.n, self.all = send, recv, 0, []
        self.peer = lambda s: {"tp": lax.rem(me + 1 + 2 * s, lax.axis_size("tp"))}

    def _make(self, at, src, dst, peer):
        return pltpu.make_async_remote_copy(src_ref=src, dst_ref=dst, send_sem=self.send.at[at], recv_sem=self.recv.at[at], device_id=peer,
                                            device_id_type=pl.DeviceIdType.MESH)

    def one(self, src, dst, peer):
        copy = self._make(self.n, src, dst, peer)
        self.n += 1
        self.all.append(copy)
        return copy

    def sides(self, refs):
        first = self.n
        self.n += 2
        get = lambda s: self._make(first + s, *refs(s), self.peer(s))
        self.all += [get(0), get(1)]
        return get

    def take(self):
        taken, self.all = _Started(self.all), []
        return taken


def _rows(i, n):
    return pl.ds(pl.multiple_of(i * n, n), n)


EXTRA = 16
PARTS = 4


def _layer(x_hbm, gain_a_hbm, gain_m_hbm, turn_hbm, wq_hbm, wk_hbm, wv_hbm, wo_hbm, wg_hbm, wu_hbm, wd_hbm, y_ref, tok, bg, bu, bd, bo, ssend, orecv,
           state, top_s, acc, hid, table, gain_a_ref, gain_m_ref, turn_ref, wsem, lsem, ssem, rsem):
    n = lax.axis_size("tp")
    me = lax.axis_index("tp")
    dp = lax.axis_index("dp")
    core, side = lax.rem(dp, 2), lax.rem(lax.div(dp, 2), 2)
    core_peer, chip_peer = {"dp": dp + 1 - 2 * core}, {"dp": dp + 2 - 4 * side}
    rows, width = x_hbm.shape
    half, quarter, part = rows // 2, rows // 4, rows // 2 // PARTS
    ff = bg.shape[1]
    columns = wq_hbm.shape[1]
    heads = columns // HEAD
    deep = HEAD + 16
    sides, tiles = (0, 1), width // TILE
    to_opp = lax.rem(me + 2, n)

    def block_of(slot):
        return lax.rem(me + (0, n - 1, 1, 2)[slot], n) if isinstance(slot, int) else lax.rem(me + n + 2 * slot - 3, n)

    w = lambda m: bg.at[:, pl.ds(m * columns, columns)]
    head = lambda ref, a: ref.at[:, a * HEAD : (a + 1) * HEAD]
    q = lambda a: bu.at[:, pl.ds(a * HEAD, HEAD)]
    k = lambda a: bu.at[:, pl.ds(columns + a * HEAD, HEAD)]
    v = lambda a: bd.at[pl.ds(a * deep, deep), :]
    low = ff - 2 * rows
    relay = lambda s: bd.at[pl.ds(low - half, half), _rows(s, columns)]
    out = lambda slot: bd.at[pl.ds(low, rows), _rows(slot, columns)]
    got = lambda slot: bd.at[pl.ds(low + rows, rows), _rows(slot, columns)]
    wo = bo
    mix = lambda bq, a: state.at[_rows(bq * heads + a, deep), :]
    halved = lambda slot: (lambda s, at=None: bo.at[slot, _rows(s, half) if at is None else _rows(s * PARTS + at, part)])
    drecv, srecv, dsend, osend = halved(0), halved(1), halved(2), halved(3)
    mid = lambda s, j: state.at[_rows(s * tiles + j, half), :]

    x = ssend
    takes = [pltpu.make_async_copy(x_hbm.at[_rows(i, half)], x.at[i], wsem.at[4 + i]) for i in (0, 1)]
    small = [pltpu.make_async_copy(hbm, ref, wsem.at[6 + i])
             for i, (hbm, ref) in enumerate(((gain_a_hbm, gain_a_ref), (gain_m_hbm, gain_m_ref), (turn_hbm, turn_ref)))]
    for take in small[:1] + takes + small[1:]:
        take.start()
    loads = [pltpu.make_async_copy(hbm, w(m), wsem.at[m]) for m, hbm in enumerate((wq_hbm, wk_hbm, wv_hbm))]
    loads.append(pltpu.make_async_copy(wo_hbm, wo.at[OWN], wsem.at[3]))
    for load in loads:
        load.start()

    def load(m, j):
        hbm, ref = ((wg_hbm, bg), (wu_hbm, bu), (wd_hbm, bd))[m]
        return pltpu.make_async_copy(hbm.at[:, _rows(j, TILE)], ref.at[:, _rows(j, TILE)], lsem.at[m, j])

    copies = _Copies(ssem, rsem, me)

    at = lambda i, p: _rows(2 * i + p, quarter)

    def own_rows(at, size):
        return lambda s: (tok.at[OWN, _rows(at(s), size)], tok.at[1 + s, _rows(at(s), size)])

    forward = lambda s: (tok.at[1 + s, _rows(s, half)], tok.at[OPP, _rows(s, half)])
    first = copies.sides(own_rows(lambda s: s, half))
    second = copies.sides(own_rows(lambda s: 1 - s, half))
    third = [copies.sides(lambda s, p=p: (tok.at[1 + s, at(s, p)], tok.at[OPP, at(s, p)])) for p in (0, 1)]
    gathered = copies.take()

    early, late, eighth = rows // 8 + EXTRA, rows // 8 - EXTRA, rows // 8

    def piece(u, t, c):
        if isinstance(t, int) and t == OPP:
            start, size = c * eighth, eighth
        else:
            s = t - 1
            start, size = (s * late, early) if c == 0 else ((1 - s) * early, late)
        return pl.ds(pl.multiple_of(u * quarter + start, 16), size)

    mine = functools.partial(piece, 2 * side + core)
    beside = functools.partial(piece, 2 * (1 - side) + core)
    wo_early = copies.sides(lambda s: (wo_hbm.at[mine(1 + s, 0)], wo.at[1 + s, mine(1 + s, 0)]))
    wo_late = copies.sides(lambda s: (wo.at[OWN, mine(1 + s, 1)], wo.at[1 + s, mine(1 + s, 1)]))
    wo_third = copies.sides(lambda s: (wo.at[1 + s, mine(OPP, s)], wo.at[OPP, mine(OPP, s)]))
    pieces = [(t, c) for t in (LEFT, RIGHT, OPP) for c in (0, 1)]
    wo_chip = {(t, c): copies.one(wo.at[t, mine(t, c)], wo.at[t, mine(t, c)], chip_peer) for t, c in pieces}
    wo_core = {(t, c): copies.one(wo.at[t, mine(t, c)], wo.at[t, mine(t, c)], core_peer) for t, c in pieces}
    wo_both = {(t, c): copies.one(wo.at[t, beside(t, c)], wo.at[t, beside(t, c)], core_peer) for t, c in pieces}
    fetched = copies.take()

    def spread(t, c):
        wo_chip[t, c].start()
        wo_core[t, c].start()

    def spread_on(t, c):
        wo_chip[t, c].wait_recv()
        wo_both[t, c].start()

    def complete(t):
        for c in (0, 1):
            wo_core[t, c].wait_recv()
            wo_both[t, c].wait_recv()

    out_o = [copies.sides(lambda s, p=p: (out(OPP).at[at(s, p)], relay(s).at[_rows(p, quarter)])) for p in (0, 1)]
    out_n = [[copies.sides(lambda s, p=p, i=i: (out(2 - s).at[at(i, p)], got(1 + s).at[at(i, p)])) for i in (0, 1)] for p in (0, 1)]
    out_f = [copies.sides(lambda s, p=p: (relay(s).at[_rows(p, quarter)], got(OPP).at[at(s, p)])) for p in (0, 1)]
    exchanged = copies.take()

    first_m = [copies.sides(own_rows(lambda s, p=p: 2 * s + p, quarter)) for p in (0, 1)]
    second_m = copies.sides(own_rows(lambda s: 1 - s, half))
    third_m = copies.sides(forward)
    direct = copies.sides(lambda s: (dsend(s), drecv(s)))
    opp = [copies.sides(lambda s, p=p: (osend(s, p), orecv.at[s, _rows(p, part)])) for p in range(PARTS)]
    total = [copies.sides(lambda s, p=p: (ssend.at[s, _rows(p, part)], srecv(s, p))) for p in range(PARTS)]
    last = copies.take()

    _greet(({"tp": lax.rem(me + 1, n)}, {"tp": lax.rem(me + n - 1, n)}, core_peer, chip_peer))
    for s in sides:
        wo_early(s).start()
    small[0].wait()
    for s in sides:
        takes[s].wait()
        _norm(x.at[s], gain_a_ref, tok.at[OWN, _rows(s, half)])
        first(s).start()
    for s in sides:
        second(s).start()
    for take in small[1:]:
        take.wait()

    def angles(block, i, t, split=False):
        place = lax.broadcasted_iota(jnp.int32, (half, HEAD), 0)
        if split:
            place = place + jnp.where(place >= quarter, quarter, 0) + (block * rows + i * quarter)
        else:
            place = place + (block * rows + i * half)
        angle = place.astype(F32) * turn_ref[...]
        sign = jnp.where(lax.broadcasted_iota(jnp.int32, (half, HEAD), 1) < HEAD // 2, -1.0, 1.0)
        table[t, 0] = jnp.cos(angle)
        table[t, 1] = jnp.sin(angle) * sign

    def project(slot, block, i, t, fresh=None, split=False):
        here = [at(0, i), at(1, i)] if split else [_rows(i, half)]
        there = [_rows(4 * block + 2 * m + i, quarter) for m in (0, 1)] if split else [_rows(2 * block + i, half)]
        size = half // len(here)

        def put(ref, axis, value):
            for m, rows_of in enumerate(there):
                if axis == 0:
                    ref[rows_of, :] = value[m * size : (m + 1) * size]
                else:
                    ref[:HEAD, rows_of] = value[:, m * size : (m + 1) * size]

        for m in range(3):
            if fresh is not None:
                pl.when(fresh)(lambda: loads[m].wait())
            some = jnp.concatenate([tok[slot, rows_of, :] for rows_of in here], axis=0)
            full = _dot(some, w(m)[...]).astype(BF16)
            for a in range(heads):
                one = full[:, a * HEAD : (a + 1) * HEAD]
                if m < 2:
                    wide = one.astype(F32)
                    put((q, k)[m](a), 0, (wide * table[t, 0] + pltpu.roll(wide, HEAD // 2, 1) * table[t, 1]).astype(BF16))
                else:
                    put(v(a), 1, one.T)

    e = HEAD**-0.5 * LOG2E

    def unit(bq, bk, masked):
        mine, here = _rows(bq, rows), _rows(bk, rows)
        scores = [_dot(k(a)[here, :], q(a)[mine, :], 1, 1) for a in range(heads)]
        weights, keeps = [], []
        for a, s in enumerate(scores):
            if masked:
                s = jnp.where(lax.broadcasted_iota(jnp.int32, s.shape, 1) >= lax.broadcasted_iota(jnp.int32, s.shape, 0), s, HIDDEN)
            old = top_s[bq, a : a + 1, :]
            top = jnp.maximum(old, s.max(axis=0, keepdims=True))
            top_s[bq, a : a + 1, :] = top
            weights.append(jnp.exp2((s - top) * e).astype(BF16))
            keeps.append(jnp.exp2((old - top) * e))
        for a, (p, keep) in enumerate(zip(weights, keeps)):
            mix(bq, a)[...] = mix(bq, a)[...] * keep + _dot(v(a)[:, here], p)

    def pair(a, b):
        unit(jnp.maximum(a, b), jnp.minimum(a, b), False)

    def finish(slot):
        block = block_of(slot)
        for a in range(heads):
            got_it = mix(block, a)[:HEAD, :] * (1 / mix(block, a)[HEAD : HEAD + 1, :])
            head(out(slot), a)[...] = got_it.T.astype(BF16)

    @pl.loop(0, n)
    def _(b):
        top_s[b] = jnp.full(top_s.shape[1:], NEG, F32)
        for a in range(heads):
            mix(b, a)[...] = jnp.zeros((deep, rows), F32)

    for a in range(heads):
        v(a)[HEAD:, :] = jnp.ones((deep - HEAD, width), BF16)

    @pl.loop(0, 2)
    def _(i):
        angles(me, i, 0)
        project(OWN, me, i, 0, fresh=i == 0)

    for s in sides:
        wo_early(s).wait_recv()
        spread(1 + s, 0)
    unit(me, me, True)

    @pl.loop(0, 2)
    def _(s):
        angles(block_of(2 - s), 1 - s, s)

    for s in sides:
        first(s).wait_recv()
        for p in (0, 1):
            third[p](s).start()

    @pl.loop(0, 2)
    def _(s):
        project(2 - s, block_of(2 - s), 1 - s, s)
        angles(block_of(2 - s), s, s)

    @pl.loop(0, 2)
    def _(s):
        second(1 - s).wait_recv()
        project(2 - s, block_of(2 - s), s, s)
        angles(to_opp, s, s, split=True)
        unit(block_of(2 - s), block_of(2 - s), True)

    @pl.loop(0, 3)
    def _(i):
        pair(lax.rem(me + n - lax.div(i, 2), n), lax.rem(me + n - 1 + 2 * jnp.minimum(i, 1), n))

    for s in sides:
        spread_on(1 + s, 0)
    loads[3].wait()
    for s in sides:
        wo_late(s).start()
        wo_third(s).start()

    def project_opposite(p):
        for s in sides:
            third[p](s).wait_recv()
        project(OPP, to_opp, p, p, split=True)

    project_opposite(0)
    project_opposite(1)

    for j in range(ff // TILE):
        load(0, j).start()
    unit(to_opp, to_opp, True)

    @pl.loop(0, 3)
    def _(i):
        pair(to_opp, lax.rem(me + n - 1 + i, n))

        @pl.when(i == 0)
        def _():
            for s in sides:
                wo_late(s).wait_recv()
                spread(1 + s, 1)

    for j in range(ff // TILE):
        load(1, j).start()
    gathered.wait_send()
    finish(OPP)
    for s in sides:
        out_o[0](s).start()
    for s in sides:
        finish(2 - s)
        for i in (0, 1):
            out_n[0][i](s).start()
    for s in sides:
        out_o[1](s).start()
    finish(OWN)
    for s in sides:
        wo_third(s).wait_recv()
        spread(OPP, s)
    for s in sides:
        out_o[0](s).wait_recv()
        out_f[0](s).start()
        for i in (0, 1):
            out_n[1][i](s).start()

    def lhs(ref, p):
        return jnp.concatenate([ref[at(i, p), :] for i in (0, 1)], axis=0)

    def most(p):
        for i in (0, 1):
            for s in sides:
                out_n[p][i](s).wait_recv()

        @pl.loop(0, tiles)
        def _(j):
            cols = _rows(j, TILE)
            t = _dot(lhs(out(OWN), p), wo[OWN, :, cols]) + _dot(lhs(got(LEFT), p), wo[LEFT, :, cols]) + _dot(lhs(got(RIGHT), p), wo[RIGHT, :, cols])
            for i in (0, 1):
                acc[at(i, p), cols] = x[i, _rows(p, quarter), cols].astype(F32) + t[i * quarter : (i + 1) * quarter]

    def rest(p):
        for s in sides:
            out_f[p](s).wait_recv()

        @pl.loop(0, tiles)
        def _(j):
            cols = _rows(j, TILE)
            t = _dot(lhs(got(OPP), p), wo[OPP, :, cols])
            for i in (0, 1):
                acc[at(i, p), cols] = (acc[at(i, p), cols] + t[i * quarter : (i + 1) * quarter]).astype(BF16).astype(F32)

        for i in (0, 1):
            _norm(acc.at[at(i, p)], gain_m_ref, tok.at[OWN, at(i, p)])
            first_m[p](i).start()

    for s in sides:
        spread_on(1 + s, 1)
    for t in (LEFT, RIGHT):
        complete(t)
    most(0)
    for s in sides:
        out_o[1](s).wait_recv()
        out_f[1](s).start()
    for c in (0, 1):
        spread_on(OPP, c)
    complete(OPP)
    rest(0)
    fetched.wait_send()
    most(1)
    rest(1)
    for s in sides:
        second_m(s).start()
    exchanged.wait_send()
    for j in range(width // TILE):
        load(2, j).start()

    def term(slot, i, store, fresh=None):
        here = _rows(i, half)

        def arrived(m, j):
            if fresh is not None:
                pl.when(fresh)(lambda: load(m, j).wait())

        @pl.loop(0, ff // TILE)
        def _(j):
            cols = _rows(j, TILE)
            arrived(0, j)
            arrived(1, j)
            gate = _dot(tok[slot, here, :], bg[:, cols])
            up = _dot(tok[slot, here, :], bu[:, cols])
            hid[:, cols] = (jax.nn.silu(gate) * up).astype(BF16)

        @pl.loop(0, tiles)
        def _(j):
            arrived(2, j)
            store(j, _dot(hid[...], bd[:, _rows(j, TILE)]))

    def put(ref):
        def store(j, t):
            ref[:, _rows(j, TILE)] = t.astype(ref.dtype)

        return store

    @pl.loop(0, 2)
    def _(i):
        def store(j, t):
            acc[_rows(i, half), _rows(j, TILE)] += t

        term(OWN, i, store, fresh=i == 0)

    for s in sides:
        for p in (0, 1):
            first_m[p](s).wait_recv()
        third_m(s).start()

    @pl.loop(0, 2)
    def _(s):
        term(2 - s, 1 - s, put(dsend(s)))
        direct(s).start()

    @pl.loop(0, 2)
    def _(s):
        def store(j, t):
            mid(s, j)[...] = t

        second_m(1 - s).wait_recv()
        term(2 - s, s, store)

    @pl.loop(0, 2)
    def _(s):
        third_m(s).wait_recv()
        term(OPP, s, put(osend(s)))
        for c in opp:
            c(s).start()

    for p in range(PARTS):
        here = _rows(p, part)
        for s in sides:
            opp[p](s).wait_recv()
            for j in range(tiles):
                cols = _rows(j, TILE)
                ssend[s, here, cols] = (mid(s, j)[here, :] + orecv[s, here, cols].astype(F32)).astype(BF16)
            total[p](s).start()
    for s in sides:
        direct(s).wait_recv()
    for p in range(PARTS):
        for s in sides:
            total[p](s).wait_recv()
            here = pl.ds(s * half + p * part, part)
            y_ref[here, :] = (acc[here, :] + srecv(s, p)[...].astype(F32) + drecv(1 - s, p)[...].astype(F32)).astype(BF16)
    last.wait_send()


def layer(x, gain_a, wq, wk, wv, wo, gain_m, w_gate, w_up, w_down):
    rows, width = x.shape
    columns, ff = wq.shape[1], w_gate.shape[1]
    heads, half = columns // HEAD, rows // 2
    tokens = 4 * rows
    if not tokens == width == ff == 4 * columns:
        raise ValueError("sizes")
    n = 56 + 2 + 4 * PARTS
    anywhere, here = pl.BlockSpec(memory_space=pl.ANY), pl.BlockSpec(memory_space=pltpu.VMEM)
    low = HEAD // 2
    turn = np.float32(THETA) ** (-np.arange(low, dtype=np.float32) / np.float32(low))
    turn = jnp.asarray(np.tile(turn, 2)[None])
    whole = lambda *shape: pltpu.VMEM(shape, BF16)
    return pl.pallas_call(
        _layer,
        out_shape=pltpu.VMEM((rows, width), BF16),
        in_specs=[anywhere] * 11,
        out_specs=here,
        scratch_shapes=[whole(4, rows, width), whole(width, ff), whole(width, ff), whole(ff, width), whole(4, columns, width),
                        whole(2, half, width), whole(2, half, width), pltpu.VMEM((4 * heads * (HEAD + 16), rows), F32),
                        pltpu.VMEM((4, heads, rows), F32), pltpu.VMEM((rows, width), F32), whole(half, ff), pltpu.VMEM((2, 2, half, HEAD), F32),
                        pltpu.VMEM(gain_a.shape, BF16), pltpu.VMEM(gain_m.shape, BF16), pltpu.VMEM(turn.shape, F32),
                        pltpu.SemaphoreType.DMA((9,)), pltpu.SemaphoreType.DMA((3, ff // TILE)), pltpu.SemaphoreType.DMA((n,)),
                        pltpu.SemaphoreType.DMA((n,))],
        compiler_params=pltpu.CompilerParams(collective_id=0, has_side_effects=True, vmem_limit_bytes=VMEM),
        cost_estimate=pl.CostEstimate(flops=8 * tokens * width * columns + 6 * tokens * width * ff, transcendentals=heads * tokens * tokens,
                                      bytes_accessed=8 * width * columns + 6 * width * ff),
        name="layer",
    )(x, gain_a, gain_m, turn, wq, wk, wv, wo, w_gate, w_up, w_down)


def solution(mesh):
    def step(x, gain_a, wq, wk, wv, wo, gain_m, w_gate, w_up, w_down):
        return layer(x, gain_a, wq, wk, wv, wo, gain_m, w_gate, w_up, w_down)

    tokens, columns, rows_of = P(("dp", "tp"), None), P(None, "tp"), P("tp", None)
    return jax.shard_map(
        step,
        mesh=mesh,
        in_specs=(tokens, P(None), columns, columns, columns, rows_of, P(None), columns, columns, rows_of),
        out_specs=tokens,
        check_vma=False,
    )
```

```python
import functools

import jax
import jax.numpy as jnp
import numpy as np
from jax import lax
from jax.experimental import pallas as pl
from jax.experimental.pallas import tpu as pltpu
from jax.sharding import PartitionSpec as P

HEAD = 128
THETA = 10000
NEG = -1e30
HIDDEN = 2 * NEG
LOG2E = 1.4426950408889634
VMEM = 67043328 - 2 * 2**20 - 2**14
TILE = 512
F32, BF16 = jnp.float32, jnp.bfloat16
OWN, LEFT, RIGHT, OPP = 0, 1, 2, 3


def _dot(a, b, ca=1, cb=0):
    return lax.dot_general(a, b, (((ca,), (cb,)), ((), ())), preferred_element_type=F32)


def _greet(peers):
    barrier = pltpu.get_barrier_semaphore()
    for peer in peers:
        pl.semaphore_signal(barrier, inc=1, device_id=peer, device_id_type=pl.DeviceIdType.MESH)
    pl.semaphore_wait(barrier, len(peers))


def _norm(src, gain_ref, dst, step=32):
    gain = gain_ref[...].astype(F32).reshape(1, -1)

    @pl.loop(0, src.shape[0] // step)
    def _(i):
        wide = src[_rows(i, step), :].astype(F32)
        scale = lax.rsqrt(jnp.mean(wide * wide, -1, keepdims=True) + 1e-6)
        dst[_rows(i, step), :] = (wide * scale * gain).astype(BF16)


class _Started:
    def __init__(self, copies):
        self.copies = copies

    def wait_send(self):
        for copy in self.copies:
            copy.wait_send()


class _Copies:
    def __init__(self, send, recv, me):
        self.send, self.recv, self.n, self.all = send, recv, 0, []
        self.peer = lambda s: {"tp": lax.rem(me + 1 + 2 * s, lax.axis_size("tp"))}

    def _make(self, at, src, dst, peer):
        return pltpu.make_async_remote_copy(src_ref=src, dst_ref=dst, send_sem=self.send.at[at], recv_sem=self.recv.at[at], device_id=peer,
                                            device_id_type=pl.DeviceIdType.MESH)

    def one(self, src, dst, peer):
        copy = self._make(self.n, src, dst, peer)
        self.n += 1
        self.all.append(copy)
        return copy

    def sides(self, refs):
        first = self.n
        self.n += 2
        get = lambda s: self._make(first + s, *refs(s), self.peer(s))
        self.all += [get(0), get(1)]
        return get

    def parts(self, n, refs):
        first = self.n
        self.n += 2 * n
        get = lambda p, s: self._make(first + 2 * p + s, *refs(p, s), self.peer(s))
        self.all += [get(p, s) for p in range(n) for s in (0, 1)]
        return get

    def take(self):
        taken, self.all = _Started(self.all), []
        return taken


def _rows(i, n):
    return pl.ds(pl.multiple_of(i * n, n), n)


EXTRA = 0
PARTS = 4


def _layer(x_hbm, gain_a_hbm, gain_m_hbm, turn_hbm, wq_hbm, wk_hbm, wv_hbm, wo_hbm, wg_hbm, wu_hbm, wd_hbm, y_ref, tok, bg, bu, bd, wo, att, orecv,
           state, top_s, gain_a_ref, gain_m_ref, turn_ref, wsem, lsem, ssem, rsem, free):
    n = lax.axis_size("tp")
    me = lax.axis_index("tp")
    dp = lax.axis_index("dp")
    core, side = lax.rem(dp, 2), lax.rem(lax.div(dp, 2), 2)
    core_peer, chip_peer = {"dp": dp + 1 - 2 * core}, {"dp": dp + 2 - 4 * side}
    rows, width = x_hbm.shape
    half, quarter, part = rows // 2, rows // 4, rows // 2 // PARTS
    ff = bg.shape[1]
    columns = wq_hbm.shape[1]
    heads = columns // HEAD
    deep = HEAD + 16
    sides, tiles = (0, 1), width // TILE
    to_opp = lax.rem(me + 2, n)

    def block_of(slot):
        return lax.rem(me + (0, n - 1, 1, 2)[slot], n) if isinstance(slot, int) else lax.rem(me + n + 2 * slot - 3, n)

    w = lambda m: bg.at[:, pl.ds(m * columns, columns)]
    q = lambda a: bu.at[:, pl.ds(a * HEAD, HEAD)]
    k = lambda a: bu.at[:, pl.ds(columns + a * HEAD, HEAD)]
    v = lambda a: bd.at[pl.ds(a * deep, deep), :]
    mix = lambda bq, a: state.at[_rows(bq * heads + a, deep), :]
    table = lambda c, m: state.at[pl.ds(n * heads * deep, quarter), _rows(2 * c + m, HEAD)]
    acc = lambda j: state.at[_rows(j, rows), :]
    nrm, hid = y_ref.at[:half, :], y_ref.at[half:, :]
    seen = lambda slot, source: att.at[slot, :, _rows(source, columns)]
    osend = lambda s: tok.at[OPP, _rows(s, half)]
    dsend = lambda s: tok.at[2 - s, _rows(1 - s, half)]
    ssend = lambda s: tok.at[2 - s, _rows(s, half)]
    drecv = lambda s: att.at[2 - s, _rows(1 - s, half)]
    srecv = lambda s: att.at[OWN, _rows(s, half)]

    takes = [pltpu.make_async_copy(x_hbm.at[_rows(i, half)], tok.at[OWN, _rows(i, half)], wsem.at[4 + i]) for i in (0, 1)]
    small = [pltpu.make_async_copy(hbm, ref, wsem.at[6 + i])
             for i, (hbm, ref) in enumerate(((gain_a_hbm, gain_a_ref), (gain_m_hbm, gain_m_ref), (turn_hbm, turn_ref)))]
    for take in small[:1] + takes + small[1:]:
        take.start()
    loads = [pltpu.make_async_copy(hbm, w(m), wsem.at[m]) for m, hbm in enumerate((wq_hbm, wk_hbm, wv_hbm))]
    loads.append(pltpu.make_async_copy(wo_hbm, wo.at[OWN], wsem.at[3]))
    for load in loads:
        load.start()

    def load(m, j):
        hbm, ref = ((wg_hbm, bg), (wu_hbm, bu), (wd_hbm, bd))[m]
        return pltpu.make_async_copy(hbm.at[:, _rows(j, TILE)], ref.at[:, _rows(j, TILE)], lsem.at[m, j])

    copies = _Copies(ssem, rsem, me)

    at = lambda i, p: _rows(2 * i + p, quarter)

    def own_rows(at, size):
        return lambda s: (tok.at[OWN, _rows(at(s), size)], tok.at[1 + s, _rows(at(s), size)])

    forward = lambda s: (tok.at[1 + s, _rows(s, half)], tok.at[OPP, _rows(s, half)])
    first = copies.sides(own_rows(lambda s: s, half))
    second = copies.sides(own_rows(lambda s: 1 - s, half))
    third = [copies.sides(lambda s, p=p: (tok.at[1 + s, at(s, p)], tok.at[OPP, at(s, p)])) for p in (0, 1)]
    gathered = copies.take()

    early, late, eighth = rows // 8 + EXTRA, rows // 8 - EXTRA, rows // 8

    def piece(u, t, c):
        if isinstance(t, int) and t == OPP:
            start, size = c * eighth, eighth
        else:
            s = t - 1
            start, size = (s * late, early) if c == 0 else ((1 - s) * early, late)
        return pl.ds(pl.multiple_of(u * quarter + start, 16), size)

    mine = functools.partial(piece, 2 * side + core)
    beside = functools.partial(piece, 2 * (1 - side) + core)
    wo_early = copies.sides(lambda s: (wo_hbm.at[mine(1 + s, 0)], wo.at[1 + s, mine(1 + s, 0)]))
    wo_late = copies.sides(lambda s: (wo.at[OWN, mine(1 + s, 1)], wo.at[1 + s, mine(1 + s, 1)]))
    wo_third = copies.sides(lambda s: (wo.at[1 + s, mine(OPP, s)], wo.at[OPP, mine(OPP, s)]))
    pieces = [(t, c) for t in (LEFT, RIGHT, OPP) for c in (0, 1)]
    wo_chip = {(t, c): copies.one(wo.at[t, mine(t, c)], wo.at[t, mine(t, c)], chip_peer) for t, c in pieces}
    wo_core = {(t, c): copies.one(wo.at[t, mine(t, c)], wo.at[t, mine(t, c)], core_peer) for t, c in pieces}
    wo_both = {(t, c): copies.one(wo.at[t, beside(t, c)], wo.at[t, beside(t, c)], core_peer) for t, c in pieces}
    fetched = copies.take()

    def spread(t, c):
        wo_chip[t, c].start()
        wo_core[t, c].start()

    def spread_on(t, c):
        wo_chip[t, c].wait_recv()
        wo_both[t, c].start()

    def complete(t):
        for c in (0, 1):
            wo_core[t, c].wait_recv()
            wo_both[t, c].wait_recv()

    names = ((LEFT, RIGHT), (RIGHT, LEFT))
    here_of = [{a: OWN, OPP: a, OWN: b, b: OPP} for a, b in names]
    sent, passed = [], []
    for s in sides:
        sent.append({(t, i): copies.one(seen(here_of[s][t], OWN).at[_rows(i, half)], seen(t, 1 + s).at[_rows(i, half)], copies.peer(s))
                     for t in range(4) for i in (0, 1)})
        passed.append({t: copies.one(seen(here_of[s][t], 1 + s).at[_rows(s, half)], seen(t, OPP).at[_rows(s, half)], copies.peer(s))
                       for t in range(4)})
    shared = copies.take()

    waited = set()

    def arrive(copy):
        if id(copy) not in waited:
            waited.add(id(copy))
            copy.wait_recv()

    def send(s, *chunks):
        for t, i in chunks:
            sent[s][t, i].start()

    def pass_on(s, t):
        arrive(sent[s][here_of[s][t], s])
        passed[s][t].start()

    def chunk_here(t, i):
        for s in sides:
            arrive(sent[s][t, i])
        arrive(passed[i][t])

    rows_of = lambda ref, p: ref.at[_rows(p, part)]
    direct = copies.sides(lambda s: (dsend(s), drecv(s)))
    opp = copies.parts(PARTS, lambda p, s: (rows_of(osend(s), p), orecv.at[s, _rows(p, part)]))
    total = copies.parts(PARTS, lambda p, s: (rows_of(ssend(s), p), rows_of(srecv(s), p)))
    last = copies.take()

    def allow(kind):
        for s in sides:
            pl.semaphore_signal(free.at[kind, s], inc=1, device_id=copies.peer(1 - s), device_id_type=pl.DeviceIdType.MESH)

    _greet(({"tp": lax.rem(me + 1, n)}, {"tp": lax.rem(me + n - 1, n)}, core_peer, chip_peer))
    for s in sides:
        wo_early(s).start()
    small[0].wait()
    for s in sides:
        takes[s].wait()
    for s in sides:
        first(s).start()
    for s in sides:
        second(s).start()
    for take in small[1:]:
        take.wait()

    def angles(block, i, split=False):
        place = lax.broadcasted_iota(jnp.int32, (half, HEAD), 0)
        if split:
            place = place + jnp.where(place >= quarter, quarter, 0) + (block * rows + i * quarter)
        else:
            place = place + (block * rows + i * half)
        angle = place.astype(F32) * turn_ref[...]
        sign = jnp.where(lax.broadcasted_iota(jnp.int32, (half, HEAD), 1) < HEAD // 2, -1.0, 1.0)
        for c, value in enumerate((jnp.cos(angle), jnp.sin(angle) * sign)):
            for m in (0, 1):
                table(c, m)[...] = value[m * quarter : (m + 1) * quarter]

    def project(slot, block, i, fresh=None, split=False):
        here = [at(0, i), at(1, i)] if split else [_rows(i, half)]
        there = [_rows(4 * block + 2 * m + i, quarter) for m in (0, 1)] if split else [_rows(2 * block + i, half)]
        size = half // len(here)

        def put(ref, axis, value):
            for m, rows_of in enumerate(there):
                if axis == 0:
                    ref[rows_of, :] = value[m * size : (m + 1) * size]
                else:
                    ref[:HEAD, rows_of] = value[:, m * size : (m + 1) * size]

        for m, rows_of in enumerate(here):
            _norm(tok.at[slot, rows_of], gain_a_ref, nrm.at[pl.ds(m * size, size)])
        for m in range(3):
            if fresh is not None:
                pl.when(fresh)(lambda: loads[m].wait())
            full = _dot(nrm[...], w(m)[...]).astype(BF16)
            cos, sin = (jnp.concatenate([table(c, z)[...] for z in (0, 1)], axis=0) for c in (0, 1))
            for a in range(heads):
                one = full[:, a * HEAD : (a + 1) * HEAD]
                if m < 2:
                    wide = one.astype(F32)
                    put((q, k)[m](a), 0, (wide * cos + pltpu.roll(wide, HEAD // 2, 1) * sin).astype(BF16))
                else:
                    put(v(a), 1, one.T)

    e = HEAD**-0.5 * LOG2E

    def unit(bq, bk, masked):
        mine, here = _rows(bq, rows), _rows(bk, rows)
        scores = [_dot(k(a)[here, :], q(a)[mine, :], 1, 1) for a in range(heads)]
        weights, keeps = [], []
        for a, s in enumerate(scores):
            if masked:
                s = jnp.where(lax.broadcasted_iota(jnp.int32, s.shape, 1) >= lax.broadcasted_iota(jnp.int32, s.shape, 0), s, HIDDEN)
            old = top_s[bq, a : a + 1, :]
            top = jnp.maximum(old, s.max(axis=0, keepdims=True))
            top_s[bq, a : a + 1, :] = top
            weights.append(jnp.exp2((s - top) * e).astype(BF16))
            keeps.append(jnp.exp2((old - top) * e))
        for a, (p, keep) in enumerate(zip(weights, keeps)):
            mix(bq, a)[...] = mix(bq, a)[...] * keep + _dot(v(a)[:, here], p)

    def pair(a, b):
        unit(jnp.maximum(a, b), jnp.minimum(a, b), False)

    def finish(slot):
        block = block_of(slot)
        for a in range(heads):
            got_it = mix(block, a)[:HEAD, :] * (1 / mix(block, a)[HEAD : HEAD + 1, :])
            att[slot, :, a * HEAD : (a + 1) * HEAD] = got_it.T.astype(BF16)

    @pl.loop(0, n)
    def _(b):
        top_s[b] = jnp.full(top_s.shape[1:], NEG, F32)
        for a in range(heads):
            mix(b, a)[...] = jnp.zeros((deep, rows), F32)

    for a in range(heads):
        v(a)[HEAD:, :] = jnp.ones((deep - HEAD, width), BF16)

    @pl.loop(0, 2)
    def _(i):
        angles(me, i)
        project(OWN, me, i, fresh=i == 0)

    for s in sides:
        wo_early(s).wait_recv()
        spread(1 + s, 0)
    unit(me, me, True)

    for s in sides:
        first(s).wait_recv()
        for p in (0, 1):
            third[p](s).start()

    @pl.loop(0, 2)
    def _(s):
        angles(block_of(2 - s), 1 - s)
        project(2 - s, block_of(2 - s), 1 - s)

    @pl.loop(0, 2)
    def _(s):
        angles(block_of(2 - s), s)
        second(1 - s).wait_recv()
        project(2 - s, block_of(2 - s), s)
        unit(block_of(2 - s), block_of(2 - s), True)

    @pl.loop(0, 3)
    def _(i):
        pair(lax.rem(me + n - lax.div(i, 2), n), lax.rem(me + n - 1 + 2 * jnp.minimum(i, 1), n))

    for s in sides:
        spread_on(1 + s, 0)
    loads[3].wait()
    for s in sides:
        wo_late(s).start()
        wo_third(s).start()

    def project_opposite(p):
        angles(to_opp, p, split=True)
        for s in sides:
            third[p](s).wait_recv()
        project(OPP, to_opp, p, split=True)

    project_opposite(0)
    project_opposite(1)

    for j in range(ff // TILE):
        load(0, j).start()
    unit(to_opp, to_opp, True)

    @pl.loop(0, 3)
    def _(i):
        pair(to_opp, lax.rem(me + n - 1 + i, n))

        @pl.when(i == 0)
        def _():
            for s in sides:
                wo_late(s).wait_recv()
                spread(1 + s, 1)

    for j in range(ff // TILE):
        load(1, j).start()
    gathered.wait_send()
    finish(OWN)
    for s, (a, b) in enumerate(names):
        send(s, (a, s))
    finish(LEFT)
    finish(RIGHT)
    for s, (a, b) in enumerate(names):
        send(s, (OPP, s), (OPP, 1 - s))
    finish(OPP)
    for j in range(tiles):
        load(2, j).start()
    for s in sides:
        wo_third(s).wait_recv()
        spread(OPP, s)
    for s in sides:
        pass_on(s, OPP)
    for s, (a, b) in enumerate(names):
        send(s, (OWN, s), (b, 1 - s), (b, s))
    for t, c in ((LEFT, 1), (RIGHT, 1), (OPP, 0), (OPP, 1)):
        spread_on(t, c)
    for t in (LEFT, RIGHT, OPP):
        complete(t)

    def term(pieces, store, fresh=None):
        size = half // len(pieces)

        def arrived(m, j):
            if fresh is not None:
                pl.when(fresh)(lambda: load(m, j).wait())

        @pl.loop(0, tiles)
        def _(j):
            cols = _rows(j, TILE)
            t = 0.0
            for source in range(4):
                some = [att[slot, at_rows, source * columns : (source + 1) * columns] for slot, at_rows in pieces]
                t = t + _dot(jnp.concatenate(some, axis=0), wo[source, :, cols])
            for m, (slot, at_rows) in enumerate(pieces):
                tok[slot, at_rows, cols] = (tok[slot, at_rows, cols].astype(F32) + t[m * size : (m + 1) * size]).astype(BF16)

        for m, (slot, at_rows) in enumerate(pieces):
            _norm(tok.at[slot, at_rows], gain_m_ref, nrm.at[pl.ds(m * size, size)])

        @pl.loop(0, ff // TILE)
        def _(j):
            cols = _rows(j, TILE)
            arrived(0, j)
            arrived(1, j)
            gate = _dot(nrm[...], bg[:, cols])
            up = _dot(nrm[...], bu[:, cols])
            hid[:, cols] = (jax.nn.silu(gate) * up).astype(BF16)

        @pl.loop(0, tiles)
        def _(j):
            arrived(2, j)
            store(j, _dot(hid[...], bd[:, _rows(j, TILE)]))

    def put(ref):
        def store(j, t):
            ref[:, _rows(j, TILE)] = t.astype(ref.dtype)

        return store

    for i in (0, 1):
        chunk_here(OPP, i)

    @pl.loop(0, 2)
    def _(s):
        term([(OPP, _rows(s, half))], put(osend(s)), fresh=s == 0)

        @pl.when(s == 0)
        def _():
            for z, (a, b) in enumerate(names):
                pass_on(z, a)
                pass_on(z, b)
                send(z, (OWN, 1 - z), (a, 1 - z))

    for s in sides:
        pass_on(s, OWN)
    for s in sides:
        for p in range(PARTS):
            opp(p, s).start()
    chunk_here(RIGHT, 1)
    chunk_here(LEFT, 0)

    @pl.loop(0, 2)
    def _(s):
        term([(2 - s, _rows(1 - s, half))], put(dsend(s)))

    shared.wait_send()
    allow(0)
    for i in (0, 1):
        chunk_here(OWN, i)

    @pl.loop(0, 2)
    def _(s):
        def store(j, t):
            acc(j)[_rows(s, half), :] = tok[OWN, _rows(s, half), _rows(j, TILE)].astype(F32) + t

        term([(OWN, _rows(s, half))], store)

        @pl.when(s == 0)
        def _():
            for z in sides:
                pl.semaphore_wait(free.at[0, z], 1)
                direct(z).start()

    allow(1)
    chunk_here(RIGHT, 0)
    chunk_here(LEFT, 1)
    for s in sides:
        pl.semaphore_wait(free.at[1, s], 1)

    @pl.loop(0, 2)
    def _(m):
        each = PARTS // 2
        for p in range(each):
            for s in sides:
                opp(m * each + p, s).wait_recv()

        def store(j, t):
            cols = _rows(j, TILE)
            for s in sides:
                came = orecv[s, _rows(m, quarter), cols].astype(F32)
                ssend(s)[_rows(m, quarter), cols] = (t[s * quarter : (s + 1) * quarter] + came).astype(BF16)

        term([(2 - s, at(s, m)) for s in sides], store)
        for p in range(each):
            for s in sides:
                total(m * each + p, s).start()

    for s in sides:
        direct(s).wait_recv()
    for p in range(PARTS):
        there = _rows(p, part)
        for s in sides:
            total(p, s).wait_recv()
            here = pl.ds(s * half + p * part, part)
            more = srecv(s)[there, :].astype(F32) + drecv(1 - s)[there, :].astype(F32)
            for j in range(tiles):
                cols = slice(j * TILE, (j + 1) * TILE)
                y_ref[here, cols] = (acc(j)[here, :] + more[:, cols]).astype(BF16)
    fetched.wait_send()
    last.wait_send()


def layer(x, gain_a, wq, wk, wv, wo, gain_m, w_gate, w_up, w_down):
    rows, width = x.shape
    columns, ff = wq.shape[1], w_gate.shape[1]
    heads, half = columns // HEAD, rows // 2
    tokens = 4 * rows
    if not tokens == width == ff == 4 * columns:
        raise ValueError("sizes")
    n = 8 + 24 + 24 + 2 + 4 * PARTS
    anywhere, here = pl.BlockSpec(memory_space=pl.ANY), pl.BlockSpec(memory_space=pltpu.VMEM)
    low = HEAD // 2
    turn = np.float32(THETA) ** (-np.arange(low, dtype=np.float32) / np.float32(low))
    turn = jnp.asarray(np.tile(turn, 2)[None])
    whole = lambda *shape: pltpu.VMEM(shape, BF16)
    return pl.pallas_call(
        _layer,
        out_shape=pltpu.VMEM((rows, width), BF16),
        in_specs=[anywhere] * 11,
        out_specs=here,
        scratch_shapes=[whole(4, rows, width), whole(width, ff), whole(width, ff), whole(ff, width), whole(4, columns, width),
                        whole(4, rows, width), whole(2, half, width), pltpu.VMEM((4 * heads * (HEAD + 16) + half // 2, rows), F32),
                        pltpu.VMEM((4, heads, rows), F32), pltpu.VMEM(gain_a.shape, BF16), pltpu.VMEM(gain_m.shape, BF16),
                        pltpu.VMEM(turn.shape, F32), pltpu.SemaphoreType.DMA((9,)), pltpu.SemaphoreType.DMA((3, ff // TILE)),
                        pltpu.SemaphoreType.DMA((n,)), pltpu.SemaphoreType.DMA((n,)), pltpu.SemaphoreType.REGULAR((2, 2))],
        compiler_params=pltpu.CompilerParams(collective_id=0, has_side_effects=True, vmem_limit_bytes=VMEM),
        cost_estimate=pl.CostEstimate(flops=8 * tokens * width * columns + 6 * tokens * width * ff, transcendentals=heads * tokens * tokens,
                                      bytes_accessed=8 * width * columns + 6 * width * ff),
        name="layer",
    )(x, gain_a, gain_m, turn, wq, wk, wv, wo, w_gate, w_up, w_down)


def solution(mesh):
    def step(x, gain_a, wq, wk, wv, wo, gain_m, w_gate, w_up, w_down):
        return layer(x, gain_a, wq, wk, wv, wo, gain_m, w_gate, w_up, w_down)

    tokens, columns, rows_of = P(("dp", "tp"), None), P(None, "tp"), P("tp", None)
    return jax.shard_map(
        step,
        mesh=mesh,
        in_specs=(tokens, P(None), columns, columns, columns, rows_of, P(None), columns, columns, rows_of),
        out_specs=tokens,
        check_vma=False,
    )
```

```python
import functools

import jax
import jax.numpy as jnp
import numpy as np
from jax import lax
from jax.experimental import pallas as pl
from jax.experimental.pallas import tpu as pltpu
from jax.sharding import PartitionSpec as P

HEAD = 128
THETA = 10000
NEG = -1e30
HIDDEN = 2 * NEG
LOG2E = 1.4426950408889634
VMEM = 67043328 - 2 * 2**20 - 2**14
TILE = 512
F32, BF16 = jnp.float32, jnp.bfloat16
OWN, LEFT, RIGHT, OPP = 0, 1, 2, 3


def _dot(a, b, ca=1, cb=0):
    return lax.dot_general(a, b, (((ca,), (cb,)), ((), ())), preferred_element_type=F32)


def _greet(peers):
    barrier = pltpu.get_barrier_semaphore()
    for peer in peers:
        pl.semaphore_signal(barrier, inc=1, device_id=peer, device_id_type=pl.DeviceIdType.MESH)
    pl.semaphore_wait(barrier, len(peers))


def _norm(src, gain_ref, dst, step=32):
    gain = gain_ref[...].astype(F32).reshape(1, -1)

    @pl.loop(0, src.shape[0] // step)
    def _(i):
        wide = src[_rows(i, step), :].astype(F32)
        scale = lax.rsqrt(jnp.mean(wide * wide, -1, keepdims=True) + 1e-6)
        dst[_rows(i, step), :] = (wide * scale * gain).astype(BF16)


class _Started:
    def __init__(self, copies):
        self.copies = copies

    def wait_send(self):
        for copy in self.copies:
            copy.wait_send()


class _Copies:
    def __init__(self, send, recv, me):
        self.send, self.recv, self.n, self.all = send, recv, 0, []
        self.peer = lambda s: {"tp": lax.rem(me + 1 + 2 * s, lax.axis_size("tp"))}

    def _make(self, at, src, dst, peer):
        return pltpu.make_async_remote_copy(src_ref=src, dst_ref=dst, send_sem=self.send.at[at], recv_sem=self.recv.at[at], device_id=peer,
                                            device_id_type=pl.DeviceIdType.MESH)

    def one(self, src, dst, peer):
        copy = self._make(self.n, src, dst, peer)
        self.n += 1
        self.all.append(copy)
        return copy

    def sides(self, refs):
        first = self.n
        self.n += 2
        get = lambda s: self._make(first + s, *refs(s), self.peer(s))
        self.all += [get(0), get(1)]
        return get

    def parts(self, n, refs):
        first = self.n
        self.n += 2 * n
        get = lambda p, s: self._make(first + 2 * p + s, *refs(p, s), self.peer(s))
        self.all += [get(p, s) for p in range(n) for s in (0, 1)]
        return get

    def take(self):
        taken, self.all = _Started(self.all), []
        return taken


def _rows(i, n):
    return pl.ds(pl.multiple_of(i * n, n), n)


EXTRA = 0
PARTS = 4


def _layer(x_hbm, gain_a_hbm, gain_m_hbm, turn_hbm, wq_hbm, wk_hbm, wv_hbm, wo_hbm, wg_hbm, wu_hbm, wd_hbm, y_ref, tok, bg, bu, bd, wo, att, orecv,
           state, top_s, gain_a_ref, gain_m_ref, turn_ref, wsem, lsem, ssem, rsem, free):
    n = lax.axis_size("tp")
    me = lax.axis_index("tp")
    dp = lax.axis_index("dp")
    core, side = lax.rem(dp, 2), lax.rem(lax.div(dp, 2), 2)
    core_peer, chip_peer = {"dp": dp + 1 - 2 * core}, {"dp": dp + 2 - 4 * side}
    rows, width = x_hbm.shape
    half, quarter, part = rows // 2, rows // 4, rows // 2 // PARTS
    ff = bg.shape[1]
    columns = wq_hbm.shape[1]
    heads = columns // HEAD
    deep = HEAD + 16
    sides, tiles = (0, 1), width // TILE
    to_opp = lax.rem(me + 2, n)

    def block_of(slot):
        return lax.rem(me + (0, n - 1, 1, 2)[slot], n) if isinstance(slot, int) else lax.rem(me + n + 2 * slot - 3, n)

    w = lambda m: bg.at[:, pl.ds(m * columns, columns)]
    q = lambda a: bu.at[:, pl.ds(a * HEAD, HEAD)]
    k = lambda a: bu.at[:, pl.ds(columns + a * HEAD, HEAD)]
    v = lambda a: bd.at[pl.ds(a * deep, deep), :]
    mix = lambda bq, a: state.at[_rows(bq * heads + a, deep), :]
    table = lambda c, m: state.at[pl.ds(n * heads * deep, quarter), _rows(2 * c + m, HEAD)]
    acc = lambda j: state.at[_rows(j, rows), :]
    nrm, hid = y_ref.at[:half, :], y_ref.at[half:, :]
    seen = lambda slot, source: att.at[slot, :, _rows(source, columns)]
    osend = lambda s: tok.at[OPP, _rows(s, half)]
    dsend = lambda s: tok.at[2 - s, _rows(1 - s, half)]
    ssend = lambda s: tok.at[2 - s, _rows(s, half)]
    drecv = lambda s: att.at[2 - s, _rows(1 - s, half)]
    srecv = lambda s: att.at[OWN, _rows(s, half)]

    takes = [pltpu.make_async_copy(x_hbm.at[_rows(i, half)], tok.at[OWN, _rows(i, half)], wsem.at[4 + i]) for i in (0, 1)]
    small = [pltpu.make_async_copy(hbm, ref, wsem.at[6 + i])
             for i, (hbm, ref) in enumerate(((gain_a_hbm, gain_a_ref), (gain_m_hbm, gain_m_ref), (turn_hbm, turn_ref)))]
    for take in small[:1] + takes + small[1:]:
        take.start()
    loads = [pltpu.make_async_copy(hbm, w(m), wsem.at[m]) for m, hbm in enumerate((wq_hbm, wk_hbm, wv_hbm))]
    loads.append(pltpu.make_async_copy(wo_hbm, wo.at[OWN], wsem.at[3]))
    for load in loads:
        load.start()

    def load(m, j):
        hbm, ref = ((wg_hbm, bg), (wu_hbm, bu), (wd_hbm, bd))[m]
        return pltpu.make_async_copy(hbm.at[:, _rows(j, TILE)], ref.at[:, _rows(j, TILE)], lsem.at[m, j])

    copies = _Copies(ssem, rsem, me)

    at = lambda i, p: _rows(2 * i + p, quarter)

    def own_rows(at, size):
        return lambda s: (tok.at[OWN, _rows(at(s), size)], tok.at[1 + s, _rows(at(s), size)])

    forward = lambda s: (tok.at[1 + s, _rows(s, half)], tok.at[OPP, _rows(s, half)])
    first = copies.sides(own_rows(lambda s: s, half))
    second = copies.sides(own_rows(lambda s: 1 - s, half))
    third = [copies.sides(lambda s, p=p: (tok.at[1 + s, at(s, p)], tok.at[OPP, at(s, p)])) for p in (0, 1)]
    gathered = copies.take()

    early, late, eighth = rows // 8 + EXTRA, rows // 8 - EXTRA, rows // 8

    def piece(u, t, c):
        if isinstance(t, int) and t == OPP:
            start, size = c * eighth, eighth
        else:
            s = t - 1
            start, size = (s * late, early) if c == 0 else ((1 - s) * early, late)
        return pl.ds(pl.multiple_of(u * quarter + start, 16), size)

    mine = functools.partial(piece, 2 * side + core)
    beside = functools.partial(piece, 2 * (1 - side) + core)
    wo_early = copies.sides(lambda s: (wo_hbm.at[mine(1 + s, 0)], wo.at[1 + s, mine(1 + s, 0)]))
    wo_late = copies.sides(lambda s: (wo.at[OWN, mine(1 + s, 1)], wo.at[1 + s, mine(1 + s, 1)]))
    wo_third = copies.sides(lambda s: (wo.at[1 + s, mine(OPP, s)], wo.at[OPP, mine(OPP, s)]))
    pieces = [(t, c) for t in (LEFT, RIGHT, OPP) for c in (0, 1)]
    wo_chip = {(t, c): copies.one(wo.at[t, mine(t, c)], wo.at[t, mine(t, c)], chip_peer) for t, c in pieces}
    wo_core = {(t, c): copies.one(wo.at[t, mine(t, c)], wo.at[t, mine(t, c)], core_peer) for t, c in pieces}
    wo_both = {(t, c): copies.one(wo.at[t, beside(t, c)], wo.at[t, beside(t, c)], core_peer) for t, c in pieces}
    fetched = copies.take()

    def spread(t, c):
        wo_chip[t, c].start()
        wo_core[t, c].start()

    def spread_on(t, c):
        wo_chip[t, c].wait_recv()
        wo_both[t, c].start()

    def complete(t):
        for c in (0, 1):
            wo_core[t, c].wait_recv()
            wo_both[t, c].wait_recv()

    names = ((LEFT, RIGHT), (RIGHT, LEFT))
    here_of = [{a: OWN, OPP: a, OWN: b, b: OPP} for a, b in names]
    sent, passed = [], []
    for s in sides:
        sent.append({(t, i): copies.one(seen(here_of[s][t], OWN).at[_rows(i, half)], seen(t, 1 + s).at[_rows(i, half)], copies.peer(s))
                     for t in range(4) for i in (0, 1)})
        passed.append({t: copies.one(seen(here_of[s][t], 1 + s).at[_rows(s, half)], seen(t, OPP).at[_rows(s, half)], copies.peer(s))
                       for t in range(4)})
    shared = copies.take()

    waited = set()

    def arrive(copy):
        if id(copy) not in waited:
            waited.add(id(copy))
            copy.wait_recv()

    def send(s, *chunks):
        for t, i in chunks:
            sent[s][t, i].start()

    def pass_on(s, t):
        arrive(sent[s][here_of[s][t], s])
        passed[s][t].start()

    def chunk_here(t, i):
        for s in sides:
            arrive(sent[s][t, i])
        arrive(passed[i][t])

    rows_of = lambda ref, p: ref.at[_rows(p, part)]
    direct = copies.sides(lambda s: (dsend(s), drecv(s)))
    opp = copies.parts(PARTS, lambda p, s: (rows_of(osend(s), p), orecv.at[s, _rows(p, part)]))
    total = copies.parts(PARTS, lambda p, s: (rows_of(ssend(s), p), rows_of(srecv(s), p)))
    last = copies.take()

    def allow(kind):
        for s in sides:
            pl.semaphore_signal(free.at[kind, s], inc=1, device_id=copies.peer(1 - s), device_id_type=pl.DeviceIdType.MESH)

    _greet(({"tp": lax.rem(me + 1, n)}, {"tp": lax.rem(me + n - 1, n)}, core_peer, chip_peer))
    for s in sides:
        wo_early(s).start()
    small[0].wait()
    for s in sides:
        takes[s].wait()
    for s in sides:
        first(s).start()
    for s in sides:
        second(s).start()
    for take in small[1:]:
        take.wait()

    def angles(block, i, split=False):
        place = lax.broadcasted_iota(jnp.int32, (half, HEAD), 0)
        if split:
            place = place + jnp.where(place >= quarter, quarter, 0) + (block * rows + i * quarter)
        else:
            place = place + (block * rows + i * half)
        angle = place.astype(F32) * turn_ref[...]
        sign = jnp.where(lax.broadcasted_iota(jnp.int32, (half, HEAD), 1) < HEAD // 2, -1.0, 1.0)
        for c, value in enumerate((jnp.cos(angle), jnp.sin(angle) * sign)):
            for m in (0, 1):
                table(c, m)[...] = value[m * quarter : (m + 1) * quarter]

    def project(slot, block, i, fresh=None, split=False):
        here = [at(0, i), at(1, i)] if split else [_rows(i, half)]
        there = [_rows(4 * block + 2 * m + i, quarter) for m in (0, 1)] if split else [_rows(2 * block + i, half)]
        size = half // len(here)

        def put(ref, axis, value):
            for m, rows_of in enumerate(there):
                if axis == 0:
                    ref[rows_of, :] = value[m * size : (m + 1) * size]
                else:
                    ref[:HEAD, rows_of] = value[:, m * size : (m + 1) * size]

        for m, rows_of in enumerate(here):
            _norm(tok.at[slot, rows_of], gain_a_ref, nrm.at[pl.ds(m * size, size)])
        for m in range(3):
            if fresh is not None:
                pl.when(fresh)(lambda: loads[m].wait())
            full = _dot(nrm[...], w(m)[...]).astype(BF16)
            cos, sin = (jnp.concatenate([table(c, z)[...] for z in (0, 1)], axis=0) for c in (0, 1))
            for a in range(heads):
                one = full[:, a * HEAD : (a + 1) * HEAD]
                if m < 2:
                    wide = one.astype(F32)
                    put((q, k)[m](a), 0, (wide * cos + pltpu.roll(wide, HEAD // 2, 1) * sin).astype(BF16))
                else:
                    put(v(a), 1, one.T)

    e = HEAD**-0.5 * LOG2E

    def unit(bq, bk, masked):
        mine, here = _rows(bq, rows), _rows(bk, rows)
        scores = [_dot(k(a)[here, :], q(a)[mine, :], 1, 1) for a in range(heads)]
        weights, keeps = [], []
        for a, s in enumerate(scores):
            if masked:
                s = jnp.where(lax.broadcasted_iota(jnp.int32, s.shape, 1) >= lax.broadcasted_iota(jnp.int32, s.shape, 0), s, HIDDEN)
            old = top_s[bq, a : a + 1, :]
            top = jnp.maximum(old, s.max(axis=0, keepdims=True))
            top_s[bq, a : a + 1, :] = top
            weights.append(jnp.exp2((s - top) * e).astype(BF16))
            keeps.append(jnp.exp2((old - top) * e))
        for a, (p, keep) in enumerate(zip(weights, keeps)):
            mix(bq, a)[...] = mix(bq, a)[...] * keep + _dot(v(a)[:, here], p)

    def pair(a, b):
        unit(jnp.maximum(a, b), jnp.minimum(a, b), False)

    def finish(slot):
        block = block_of(slot)
        for a in range(heads):
            got_it = mix(block, a)[:HEAD, :] * (1 / mix(block, a)[HEAD : HEAD + 1, :])
            att[slot, :, a * HEAD : (a + 1) * HEAD] = got_it.T.astype(BF16)

    @pl.loop(0, n)
    def _(b):
        top_s[b] = jnp.full(top_s.shape[1:], NEG, F32)
        for a in range(heads):
            mix(b, a)[...] = jnp.zeros((deep, rows), F32)

    for a in range(heads):
        v(a)[HEAD:, :] = jnp.ones((deep - HEAD, width), BF16)

    @pl.loop(0, 2)
    def _(i):
        angles(me, i)
        project(OWN, me, i, fresh=i == 0)

    for s in sides:
        wo_early(s).wait_recv()
        spread(1 + s, 0)
    unit(me, me, True)

    for s in sides:
        first(s).wait_recv()
        for p in (0, 1):
            third[p](s).start()

    @pl.loop(0, 2)
    def _(s):
        angles(block_of(2 - s), 1 - s)
        project(2 - s, block_of(2 - s), 1 - s)

    @pl.loop(0, 2)
    def _(s):
        angles(block_of(2 - s), s)
        second(1 - s).wait_recv()
        project(2 - s, block_of(2 - s), s)
        unit(block_of(2 - s), block_of(2 - s), True)

    @pl.loop(0, 3)
    def _(i):
        pair(lax.rem(me + n - lax.div(i, 2), n), lax.rem(me + n - 1 + 2 * jnp.minimum(i, 1), n))

    for s in sides:
        spread_on(1 + s, 0)
    loads[3].wait()
    for s in sides:
        wo_late(s).start()
        wo_third(s).start()

    def project_opposite(p):
        angles(to_opp, p, split=True)
        for s in sides:
            third[p](s).wait_recv()
        project(OPP, to_opp, p, split=True)

    project_opposite(0)
    project_opposite(1)

    for j in range(ff // TILE):
        load(0, j).start()
    unit(to_opp, to_opp, True)

    @pl.loop(0, 3)
    def _(i):
        pair(to_opp, lax.rem(me + n - 1 + i, n))

        @pl.when(i == 0)
        def _():
            for s in sides:
                wo_late(s).wait_recv()
                spread(1 + s, 1)

    for j in range(ff // TILE):
        load(1, j).start()
    gathered.wait_send()
    finish(OWN)
    for s, (a, b) in enumerate(names):
        send(s, (a, s))
    finish(LEFT)
    finish(RIGHT)
    for s, (a, b) in enumerate(names):
        send(s, (OPP, s), (OPP, 1 - s))
    finish(OPP)
    for j in range(tiles):
        load(2, j).start()
    for s in sides:
        wo_third(s).wait_recv()
        spread(OPP, s)
    for s in sides:
        pass_on(s, OPP)
    for s, (a, b) in enumerate(names):
        send(s, (OWN, s), (b, 1 - s), (b, s))
    for t, c in ((LEFT, 1), (RIGHT, 1), (OPP, 0), (OPP, 1)):
        spread_on(t, c)
    for t in (LEFT, RIGHT, OPP):
        complete(t)

    def term(pieces, store, fresh=None):
        size = half // len(pieces)

        def arrived(m, j):
            if fresh is not None:
                pl.when(fresh)(lambda: load(m, j).wait())

        @pl.loop(0, tiles)
        def _(j):
            cols = _rows(j, TILE)
            some = jnp.concatenate([att[slot, at_rows, :] for slot, at_rows in pieces], axis=0)
            t = _dot(some, wo[:, :, cols].reshape(4 * columns, TILE))
            for m, (slot, at_rows) in enumerate(pieces):
                tok[slot, at_rows, cols] = (tok[slot, at_rows, cols].astype(F32) + t[m * size : (m + 1) * size]).astype(BF16)

        for m, (slot, at_rows) in enumerate(pieces):
            _norm(tok.at[slot, at_rows], gain_m_ref, nrm.at[pl.ds(m * size, size)])

        @pl.loop(0, ff // TILE)
        def _(j):
            cols = _rows(j, TILE)
            arrived(0, j)
            arrived(1, j)
            gate = _dot(nrm[...], bg[:, cols])
            up = _dot(nrm[...], bu[:, cols])
            hid[:, cols] = (jax.nn.silu(gate) * up).astype(BF16)

        @pl.loop(0, tiles)
        def _(j):
            arrived(2, j)
            store(j, _dot(hid[...], bd[:, _rows(j, TILE)]))

    def put(ref):
        def store(j, t):
            ref[:, _rows(j, TILE)] = t.astype(ref.dtype)

        return store

    for i in (0, 1):
        chunk_here(OPP, i)

    @pl.loop(0, 2)
    def _(s):
        term([(OPP, _rows(s, half))], put(osend(s)), fresh=s == 0)

        @pl.when(s == 0)
        def _():
            for z, (a, b) in enumerate(names):
                pass_on(z, a)
                pass_on(z, b)
                send(z, (OWN, 1 - z), (a, 1 - z))

    for s in sides:
        pass_on(s, OWN)
    for s in sides:
        for p in range(PARTS):
            opp(p, s).start()
    chunk_here(RIGHT, 1)
    chunk_here(LEFT, 0)

    @pl.loop(0, 2)
    def _(s):
        term([(2 - s, _rows(1 - s, half))], put(dsend(s)))

    shared.wait_send()
    allow(0)
    for i in (0, 1):
        chunk_here(OWN, i)

    @pl.loop(0, 2)
    def _(s):
        def store(j, t):
            acc(j)[_rows(s, half), :] = tok[OWN, _rows(s, half), _rows(j, TILE)].astype(F32) + t

        term([(OWN, _rows(s, half))], store)

        @pl.when(s == 0)
        def _():
            for z in sides:
                pl.semaphore_wait(free.at[0, z], 1)
                direct(z).start()

    allow(1)
    chunk_here(RIGHT, 0)
    chunk_here(LEFT, 1)

    @pl.loop(0, 2)
    def _(m):
        each = PARTS // 2
        for p in range(each):
            for s in sides:
                opp(m * each + p, s).wait_recv()

        def store(j, t):
            cols = _rows(j, TILE)
            for s in sides:
                came = orecv[s, _rows(m, quarter), cols].astype(F32)
                ssend(s)[_rows(m, quarter), cols] = (t[s * quarter : (s + 1) * quarter] + came).astype(BF16)

        term([(2 - s, at(s, m)) for s in sides], store)

        @pl.when(m == 0)
        def _():
            for z in sides:
                pl.semaphore_wait(free.at[1, z], 1)

        for p in range(each):
            for s in sides:
                total(m * each + p, s).start()

    for s in sides:
        direct(s).wait_recv()
    for p in range(PARTS):
        there = _rows(p, part)
        for s in sides:
            total(p, s).wait_recv()
            here = pl.ds(s * half + p * part, part)
            more = srecv(s)[there, :].astype(F32) + drecv(1 - s)[there, :].astype(F32)
            for j in range(tiles):
                cols = slice(j * TILE, (j + 1) * TILE)
                y_ref[here, cols] = (acc(j)[here, :] + more[:, cols]).astype(BF16)
    fetched.wait_send()
    last.wait_send()


def layer(x, gain_a, wq, wk, wv, wo, gain_m, w_gate, w_up, w_down):
    rows, width = x.shape
    columns, ff = wq.shape[1], w_gate.shape[1]
    heads, half = columns // HEAD, rows // 2
    tokens = 4 * rows
    if not tokens == width == ff == 4 * columns:
        raise ValueError("sizes")
    n = 8 + 24 + 24 + 2 + 4 * PARTS
    anywhere, here = pl.BlockSpec(memory_space=pl.ANY), pl.BlockSpec(memory_space=pltpu.VMEM)
    low = HEAD // 2
    turn = np.float32(THETA) ** (-np.arange(low, dtype=np.float32) / np.float32(low))
    turn = jnp.asarray(np.tile(turn, 2)[None])
    whole = lambda *shape: pltpu.VMEM(shape, BF16)
    return pl.pallas_call(
        _layer,
        out_shape=pltpu.VMEM((rows, width), BF16),
        in_specs=[anywhere] * 11,
        out_specs=here,
        scratch_shapes=[whole(4, rows, width), whole(width, ff), whole(width, ff), whole(ff, width), whole(4, columns, width),
                        whole(4, rows, width), whole(2, half, width), pltpu.VMEM((4 * heads * (HEAD + 16) + half // 2, rows), F32),
                        pltpu.VMEM((4, heads, rows), F32), pltpu.VMEM(gain_a.shape, BF16), pltpu.VMEM(gain_m.shape, BF16),
                        pltpu.VMEM(turn.shape, F32), pltpu.SemaphoreType.DMA((9,)), pltpu.SemaphoreType.DMA((3, ff // TILE)),
                        pltpu.SemaphoreType.DMA((n,)), pltpu.SemaphoreType.DMA((n,)), pltpu.SemaphoreType.REGULAR((2, 2))],
        compiler_params=pltpu.CompilerParams(collective_id=0, has_side_effects=True, vmem_limit_bytes=VMEM),
        cost_estimate=pl.CostEstimate(flops=8 * tokens * width * columns + 6 * tokens * width * ff, transcendentals=heads * tokens * tokens,
                                      bytes_accessed=8 * width * columns + 6 * width * ff),
        name="layer",
    )(x, gain_a, gain_m, turn, wq, wk, wv, wo, w_gate, w_up, w_down)


def solution(mesh):
    def step(x, gain_a, wq, wk, wv, wo, gain_m, w_gate, w_up, w_down):
        return layer(x, gain_a, wq, wk, wv, wo, gain_m, w_gate, w_up, w_down)

    tokens, columns, rows_of = P(("dp", "tp"), None), P(None, "tp"), P("tp", None)
    return jax.shard_map(
        step,
        mesh=mesh,
        in_specs=(tokens, P(None), columns, columns, columns, rows_of, P(None), columns, columns, rows_of),
        out_specs=tokens,
        check_vma=False,
    )
```
